32 devices in a mesh: sub: 16 (over z, x, core), row: 2 (over y).
Axes of the slice: x: 2, y: 2, z: 4, core: 2. Of those that a mesh axis runs over, the one named last changes fastest.
Arguments:
- factor_blocks: float32 [16, 8, 3, 256, 256], P('sub', 'row'), may hold values from -0.25 to 0.25
- block_inverses: float32 [16, 8, 256, 256], P('sub', 'row'), as said below
- band_offsets: int32 [16, 8, 3], P('sub', 'row'), may hold values from 1 to 4, as said below
- coupling: float32 [16, 2048, 512], P('sub', 'row'), may hold values from -0.125 to 0.125
- interface_block: float32 [16, 4, 128, 512], P('sub', None, 'row'), may hold values from -6 to 6
- tile_ids: int32 [16, 4], replicated, may hold values from 0 to 127, as said below
Outputs:
- schur_tiles: float32 [16, 4, 128, 512], P('sub', None, 'row')
The draws below stay inside these ranges and needn't reach their ends.
Inputs may be any that keep to these rules, and one draw needn't show every extreme that they name: `band_offsets`: each entry is one of the numbers 1 .. 4, the 3 entries of a block row are distinct and rising. `tile_ids`: A subdomain's 4 numbers are distinct; a number appears in at most two subdomains, and then in neighbouring ones (s and s + 1); every subdomain but the last shares one or two numbers with the next. `block_inverses`: each block is lower triangular with a diagonal between 0.5 and 1.
All inputs are finite; a program needn't handle non-finite values.
Results may differ from the reference program's by a relative error of at most 0.0003.
Values sent between devices are 32-bit elements; how exact they have to be, the bound alone decides.
No kernel may reach another device: no remote copies, remote signals or barrier semaphores. Data moves between devices by JAX's collectives and lax.ppermute only.
A program may use at most 64 MiB of HBM per device.

```python
import jax
import jax.numpy as jnp
from jax import lax

BLK = 256
K = 3
P_SIZE = 512
TILE = 128
TILES = 4
NB = 8
NI = 2048
SUBS = 16


def draw_block_inverses(key, part):
    key_diag, key_low = jax.random.split(jax.random.fold_in(key, 11))
    shape = (SUBS, NB, BLK, BLK)
    diagonal = jnp.exp(jax.random.uniform(key_diag, (SUBS, NB, BLK), jnp.float32, jnp.log(0.5), 0.0))
    lower = jax.random.normal(key_low, shape, jnp.float32) * (0.5 / BLK ** 0.5)
    strict = jnp.tril(lower, -1)
    return strict + jnp.eye(BLK, dtype=jnp.float32) * diagonal[..., None]


def draw_band_offsets(key, part):
    excluded = jax.random.randint(jax.random.fold_in(key, 23), (SUBS, NB), 1, K + 2)
    base = jnp.arange(1, K + 1, dtype=jnp.int32)
    return (base + (base >= excluded[..., None]).astype(jnp.int32)).astype(jnp.int32)


def draw_tile_ids(key, part):
    key_share, key_order = jax.random.split(jax.random.fold_in(key, 37))
    positions = jnp.arange(SUBS, dtype=jnp.int32)
    shared = jax.random.randint(key_share, (SUBS,), 1, 3)
    shared = jnp.where(positions == SUBS - 1, 0, shared)
    left = jnp.concatenate([jnp.zeros((1,), jnp.int32), shared[:-1]])
    slots = jnp.arange(TILES, dtype=jnp.int32)[None, :]
    owner = positions[:, None]
    left_id = 2 * TILES * (owner - 1) + TILES + slots
    private_id = 2 * TILES * owner + (slots - left[:, None])
    right_id = 2 * TILES * owner + TILES + (slots - (TILES - shared[:, None]))
    ordered = jnp.where(slots < left[:, None], left_id, jnp.where(slots < TILES - shared[:, None], private_id, right_id))
    scores = jax.random.randint(key_order, (SUBS, TILES), 0, 2 ** 20) * TILES + slots
    order = jnp.argsort(scores, axis=1)
    return jnp.take_along_axis(ordered, order, axis=1).astype(jnp.int32)


def shard_levels(stream_key, shape, cuts, least, top_value):
    gain = 1.0
    for axis_at, blocks in cuts:
        steps = jax.random.uniform(jax.random.fold_in(jax.random.fold_in(stream_key, 6), axis_at), (blocks,), jnp.float32, least / len(cuts), top_value / len(cuts))
        gain = gain * jnp.repeat(jnp.exp(steps), shape[axis_at] // blocks).reshape((-1,) + (1,) * (len(shape) - 1 - axis_at))
    return gain


def gaussian(rng, extent, scale, bound, cuts=(), kind=jnp.bfloat16):
    drawn = scale * jax.random.normal(rng, extent, jnp.float32)
    if cuts:
        drawn = drawn * shard_levels(rng, extent, cuts, -0.22, 0.18)
    return jnp.clip(drawn, -bound, bound).astype(kind)


def setup_inputs(seed: int = 0) -> dict:
    splits = jax.random.split(jax.random.key(seed), 7)
    return {
        "factor_blocks": gaussian(splits[0], (SUBS, NB, K, BLK, BLK), (5 * BLK // 2) ** -0.5, 0.25, ((0, 16), (1, 2)), jnp.float32),
        "block_inverses": draw_block_inverses(jax.random.fold_in(splits[6], 71), 0),
        "band_offsets": draw_band_offsets(jax.random.fold_in(splits[6], 71), 0),
        "coupling": gaussian(splits[3], (SUBS, NI, P_SIZE), NI ** -0.5, 0.125, ((0, 16), (1, 2)), jnp.float32),
        "interface_block": gaussian(splits[4], (SUBS, TILES, TILE, P_SIZE), 1.0, 6.0, ((0, 16), (2, 2)), jnp.float32),
        "tile_ids": draw_tile_ids(jax.random.fold_in(splits[6], 71), 0),
    }


def solve_subdomain(blocks, inverses, offsets, coupling):
    right_side = coupling.reshape(NB, BLK, P_SIZE)
    padded = jnp.zeros((NB + K + 1, BLK, P_SIZE), jnp.float32)

    def substitute(row_block, padded):
        running = lax.dynamic_index_in_dim(right_side, row_block, 0, keepdims=False)
        factor_row = lax.dynamic_index_in_dim(blocks, row_block, 0, keepdims=False)
        offset_row = lax.dynamic_index_in_dim(offsets, row_block, 0, keepdims=False)
        for band in range(K):
            source_index = (row_block + K + 1 - offset_row[band]).astype(jnp.int32)
            source = lax.dynamic_index_in_dim(padded, source_index, 0, keepdims=False)
            running = running - jnp.dot(factor_row[band], source, precision=lax.Precision.HIGHEST)
        inverse = lax.dynamic_index_in_dim(inverses, row_block, 0, keepdims=False)
        solved_row = jnp.dot(inverse, running, precision=lax.Precision.HIGHEST)
        target = (row_block + K + 1).astype(jnp.int32)
        return lax.dynamic_update_index_in_dim(padded, solved_row, target, 0)

    padded = lax.fori_loop(jnp.int32(0), jnp.int32(NB), substitute, padded)
    flattened = padded[K + 1:].reshape(NI, P_SIZE)
    gram = lax.dot_general(flattened, flattened, (((0,), (0,)), ((), ())), precision=lax.Precision.HIGHEST)
    return gram.reshape(TILES, TILE, P_SIZE)


def reference(factor_blocks, block_inverses, band_offsets, coupling, interface_block, tile_ids):
    grams = lax.map(lambda args: solve_subdomain(*args), (factor_blocks, block_inverses, band_offsets, coupling))
    zero_gram = jnp.zeros((1, TILES, TILE, P_SIZE), jnp.float32)
    padded_grams = jnp.concatenate([zero_gram, grams, zero_gram], 0)
    positions = jnp.arange(SUBS, dtype=jnp.int32)
    contribution = jnp.zeros((SUBS, TILES, TILE, TILES, TILE), jnp.float32)
    for delta in range(3):
        neighbour_gram = padded_grams[delta:delta + SUBS].reshape(SUBS, TILES, TILE, TILES, TILE)
        neighbour_pos = jnp.clip(positions + delta - 1, 0, SUBS - 1).astype(jnp.int32)
        neighbour_ids = tile_ids[neighbour_pos]
        match = (tile_ids[:, :, None] == neighbour_ids[:, None, :]).astype(jnp.float32)
        contribution = contribution + jnp.einsum('sik,sjl,skalb->siajb', match, match, neighbour_gram, precision=lax.Precision.HIGHEST)
    return interface_block - contribution.reshape(SUBS, TILES, TILE, P_SIZE)
```

```python
import functools

import jax
import jax.numpy as jnp
from jax import lax
from jax.experimental import pallas as pl
from jax.experimental.pallas import tpu as pltpu
from jax.sharding import PartitionSpec as P


F32 = jnp.float32
BF16 = jnp.bfloat16
VMEM_LIMIT = 24 * 1024 * 1024
SLOTS = 2


def split(x):
    high = x.astype(BF16)
    return high, (x - high.astype(F32)).astype(BF16)


def nt(a, b):
    return lax.dot_general(a, b, (((1,), (1,)), ((), ())), preferred_element_type=F32)


def nn(a, b):
    return lax.dot_general(a, b, (((1,), (0,)), ((), ())), preferred_element_type=F32)


def three(dot, a, b):
    return dot(a[0], b[0]) + (dot(a[0], b[1]) + dot(a[1], b[0]))


def solve_kernel(off_ref, f_ref, inv_ref, b_ref, *rest, chunks):
    outs, (high, low, acc) = rest[: len(chunks)], rest[len(chunks) :]
    i = pl.program_id(0)
    acc[...] = b_ref[0].T
    for band in range(f_ref.shape[2]):
        source = i - off_ref[0, i, band]

        @pl.when(source >= 0)
        def _():
            acc[...] -= three(nt, (high[source], low[source]), split(f_ref[0, 0, band]))

    x = three(nt, split(acc[...]), split(inv_ref[0, 0]))
    high[i], low[i] = split(x)
    start = 0
    for out, size in zip(outs, chunks):
        out[...] = x[start : start + size]
        start += size


def solve(offsets, blocks, inverses, coupling, chunks):
    _, brows, kband, size, _ = blocks.shape
    cols = coupling.shape[2]
    return pl.pallas_call(
        functools.partial(solve_kernel, chunks=chunks),
        grid=(brows,),
        in_specs=[
            pl.BlockSpec(memory_space=pltpu.SMEM),
            pl.BlockSpec((1, 1, kband, size, size), lambda i: (0, i, 0, 0, 0)),
            pl.BlockSpec((1, 1, size, size), lambda i: (0, i, 0, 0)),
            pl.BlockSpec((1, size, cols), lambda i: (0, i, 0)),
        ],
        out_specs=[pl.BlockSpec((n, size), lambda i: (0, i)) for n in chunks],
        out_shape=[jax.ShapeDtypeStruct((n, brows * size), F32) for n in chunks],
        scratch_shapes=[
            pltpu.VMEM((brows, cols, size), BF16),
            pltpu.VMEM((brows, cols, size), BF16),
            pltpu.VMEM((cols, size), F32),
        ],
        compiler_params=pltpu.CompilerParams(vmem_limit_bytes=VMEM_LIMIT),
        cost_estimate=pl.CostEstimate(flops=6 * 10 * size * size * cols, bytes_accessed=8 << 20, transcendentals=0),
        name="solve",
    )(offsets, blocks, inverses, coupling)


def response_kernel(off_ref, f_ref, inv_ref, gh_ref, gl_ref, high, low, acc):
    i = pl.program_id(0)
    brows, size = high.shape[0], high.shape[1]

    @pl.when(lax.axis_index("row") > 0)
    def _():
        acc[...] = jnp.zeros_like(acc)
        for band in range(f_ref.shape[2]):
            source = i - off_ref[0, i, band]

            @pl.when(source < 0)
            def _():
                at = pl.multiple_of((source + brows) * size, size)
                acc[:, pl.ds(at, size)] += f_ref[0, 0, band]

            @pl.when(source >= 0)
            def _():
                acc[...] -= three(nn, split(f_ref[0, 0, band]), (high[source], low[source]))

        g = three(nn, split(inv_ref[0, 0]), split(acc[...]))
        gh, gl = split(g)
        high[i], low[i] = gh, gl
        gh_ref[...] = gh
        gl_ref[...] = gl


def response(offsets, blocks, inverses):
    _, brows, kband, size, _ = blocks.shape
    width = brows * size
    return pl.pallas_call(
        response_kernel,
        grid=(brows,),
        in_specs=[
            pl.BlockSpec(memory_space=pltpu.SMEM),
            pl.BlockSpec((1, 1, kband, size, size), lambda i: (0, i, 0, 0, 0)),
            pl.BlockSpec((1, 1, size, size), lambda i: (0, i, 0, 0)),
        ],
        out_specs=[pl.BlockSpec((size, width), lambda i: (i, 0))] * 2,
        out_shape=[jax.ShapeDtypeStruct((width, width), BF16)] * 2,
        scratch_shapes=[
            pltpu.VMEM((brows, size, width), BF16),
            pltpu.VMEM((brows, size, width), BF16),
            pltpu.VMEM((size, width), F32),
        ],
        compiler_params=pltpu.CompilerParams(vmem_limit_bytes=VMEM_LIMIT),
        cost_estimate=pl.CostEstimate(flops=6 * 10 * size * size * width, bytes_accessed=8 << 20, transcendentals=0),
        name="response",
    )(offsets, blocks, inverses)


def update_kernel(recv_ref, y_ref, cur_ref, gh_ref, gl_ref, out_ref, *, stage):
    out_ref[...] = cur_ref[...]

    @pl.when(lax.axis_index("row") == stage)
    def _():
        out_ref[...] = y_ref[...] - three(nt, split(recv_ref[...]), (gh_ref[...], gl_ref[...]))


def update(recv, y, cur, gain, stage):
    return pl.pallas_call(
        functools.partial(update_kernel, stage=stage),
        out_shape=jax.ShapeDtypeStruct(y.shape, F32),
        compiler_params=pltpu.CompilerParams(vmem_limit_bytes=VMEM_LIMIT),
        name="update",
    )(recv, y, cur, *gain)


def gram_kernel(*refs, at, fused, parts, share):
    recv_ref, y_ref = refs[:2]
    refs = refs[2:]
    if fused:
        gh_ref, gl_ref = refs[:2]
        refs = refs[2:]
    earlier, refs = refs[: 2 * at], refs[2 * at :]
    zh_ref, zl_ref = refs[:2]
    pieces = refs[2:]
    half = recv_ref.shape[1]

    @pl.when(lax.axis_index("row") > 0)
    def _():
        rh, rl = split(recv_ref[...])
        x = y_ref[...]
        if fused:
            x = x - three(nt, (rh, rl), (gh_ref[...], gl_ref[...]))
        xh, xl = split(x)
        zh_ref[:, :half], zl_ref[:, :half] = rh, rl
        zh_ref[:, half:], zl_ref[:, half:] = xh, xl
        mine = (zh_ref[...], zl_ref[...])
        for t in range(at + 1):
            other = (earlier[2 * t][...], earlier[2 * t + 1][...]) if t < at else mine
            block = three(nt, other, mine)
            for part in range(parts):
                rows = slice(part * share, (part + 1) * share)
                pieces[part][t * share : (t + 1) * share] = block[rows]
            if t < at:
                turned = block.T
                for part in range(parts):
                    rows = slice(part * share, (part + 1) * share)
                    first = (at + 1 + t) * share
                    pieces[part][first : first + share] = turned[rows]

    if parts > 2:

        @pl.when(lax.axis_index("row") == 0)
        def _():
            for piece in pieces:
                piece[...] = jnp.zeros_like(piece)


def gram(recv, y, gain, earlier, parts):
    tile, half = y.shape
    at = len(earlier) // 2
    share = tile // parts
    fused = bool(gain)
    results = pl.pallas_call(
        functools.partial(gram_kernel, at=at, fused=fused, parts=parts, share=share),
        out_shape=[jax.ShapeDtypeStruct((tile, 2 * half), BF16)] * 2
        + [jax.ShapeDtypeStruct(((2 * at + 1) * share, tile), F32)] * parts,
        compiler_params=pltpu.CompilerParams(vmem_limit_bytes=VMEM_LIMIT),
        cost_estimate=pl.CostEstimate(
            flops=6 * tile * half * (half + 2 * tile * (at + 1)), bytes_accessed=4 << 20, transcendentals=0
        ),
        name=f"gram{at}",
    )(recv, y, *gain, *earlier)
    return list(results[:2]), list(results[2:])


def shared_slots(ids, mine, other, count):
    total = ids.shape[0]
    inside = jnp.logical_and(
        jnp.logical_and(mine >= 0, mine < total), jnp.logical_and(other >= 0, other < total)
    )
    mine, other = jnp.clip(mine, 0, total - 1), jnp.clip(other, 0, total - 1)
    found = jnp.int32(0)
    slots = [[jnp.int32(0), jnp.int32(0), jnp.bool_(False)] for _ in range(SLOTS)]
    for k in range(count):
        hit, place = jnp.bool_(False), jnp.int32(0)
        for i in range(count):
            same = ids[mine, k] == ids[other, i]
            hit = jnp.logical_or(hit, same)
            place = jnp.where(same, jnp.int32(i), place)
        hit = jnp.logical_and(hit, inside)
        for m, slot in enumerate(slots):
            take = jnp.logical_and(hit, found == m)
            slot[0] = jnp.where(take, jnp.int32(k), slot[0])
            slot[1] = jnp.where(take, place, slot[1])
            slot[2] = jnp.logical_or(slot[2], take)
        found = found + hit.astype(jnp.int32)
    return slots


def collect_kernel(ids_ref, face_ref, *refs, count, exchanged):
    pieces, (base_ref, left_ref, right_ref, g) = refs[:-4], refs[-4:]
    _, share, cols = g.shape
    tile = cols // count
    row, sub = lax.axis_index("row"), lax.axis_index("sub")

    def fill(pieces):
        for c, piece in enumerate(pieces):
            for t in range(c + 1):
                g[t, :, c * tile : (c + 1) * tile] = piece[t * share : (t + 1) * share]
            for t in range(c):
                first = (c + 1 + t) * share
                g[c, :, t * tile : (t + 1) * tile] = piece[first : first + share]

    if exchanged:
        pl.when(row == 0)(lambda: fill(pieces[:count]))
        pl.when(row != 0)(lambda: fill(pieces[count:]))
    else:
        fill(pieces)
    base_ref[...] = face_ref[0] - g[...]
    for delta, out in ((-1, left_ref), (1, right_ref)):
        slots = shared_slots(ids_ref, sub, sub + delta, count)
        for m in range(SLOTS):
            for n in range(SLOTS):
                at = pl.multiple_of(slots[n][0] * tile, tile)
                out[m, :, n * tile : (n + 1) * tile] = g[slots[m][0], :, pl.ds(at, tile)]


def collect(ids, face, pieces, exchanged):
    _, count, share, cols = face.shape
    smem = pl.BlockSpec(memory_space=pltpu.SMEM)
    vmem = pl.BlockSpec(memory_space=pltpu.VMEM)
    halo = jax.ShapeDtypeStruct((SLOTS, share, SLOTS * (cols // count)), F32)
    return pl.pallas_call(
        functools.partial(collect_kernel, count=count, exchanged=exchanged),
        in_specs=[smem, vmem] + [vmem] * len(pieces),
        out_shape=[jax.ShapeDtypeStruct((count, share, cols), F32), halo, halo],
        scratch_shapes=[pltpu.VMEM((count, share, cols), F32)],
        compiler_params=pltpu.CompilerParams(vmem_limit_bytes=VMEM_LIMIT),
        name="collect",
    )(ids, face, *pieces)


def finish_kernel(ids_ref, base_ref, left_ref, right_ref, out_ref, *, count):
    cols = base_ref.shape[2]
    tile = cols // count
    sub = lax.axis_index("sub")
    out_ref[0] = base_ref[...]
    for delta, halo in ((-1, left_ref), (1, right_ref)):
        slots = shared_slots(ids_ref, sub + delta, sub, count)
        for m in range(SLOTS):
            for n in range(SLOTS):

                @pl.when(jnp.logical_and(slots[m][2], slots[n][2]))
                def _():
                    at = pl.multiple_of(slots[n][1] * tile, tile)
                    out_ref[0, slots[m][1], :, pl.ds(at, tile)] -= halo[m, :, n * tile : (n + 1) * tile]


def finish(ids, base, left, right):
    count, share, cols = base.shape
    smem = pl.BlockSpec(memory_space=pltpu.SMEM)
    vmem = pl.BlockSpec(memory_space=pltpu.VMEM)
    return pl.pallas_call(
        functools.partial(finish_kernel, count=count),
        in_specs=[smem, vmem, vmem, vmem],
        out_shape=jax.ShapeDtypeStruct((1, count, share, cols), F32),
        compiler_params=pltpu.CompilerParams(vmem_limit_bytes=VMEM_LIMIT),
        name="finish",
    )(ids, base, left, right)


def shards(factor_blocks, block_inverses, band_offsets, coupling, interface_block, tile_ids):
    rows = lax.axis_size("row")
    subs = lax.axis_size("sub")
    count = interface_block.shape[1]
    tile = coupling.shape[2] // count
    chunks = (tile,) * count
    ys = solve(band_offsets, factor_blocks, block_inverses, coupling, chunks)
    gain = response(band_offsets, factor_blocks, block_inverses)
    if rows == 2:
        first = [lax.ppermute(y, "row", [(0, 1)]) for y in ys]
        xs, gain_now = ys, gain
    else:
        xs, first, gain_now = list(ys), None, ()
        for stage in range(1, rows):
            recv = [lax.ppermute(x, "row", [(stage - 1, stage)]) for x in xs]
            first = first or recv
            xs = [update(r, y, x, gain, stage) for r, y, x in zip(recv, ys, xs)]
    earlier, own, got = [], [], []
    for recv, x in zip(first, xs):
        z, pieces = gram(recv, x, gain_now, earlier, rows)
        earlier = earlier + z
        if rows == 2:
            got.append(lax.ppermute(pieces[0], "row", [(1, 0)]))
            own.append(pieces[1])
        else:
            own.append(lax.psum_scatter(jnp.stack(pieces), "row", scatter_dimension=0, tiled=False))
    base, left, right = collect(tile_ids, interface_block, got + own, rows == 2)
    from_left = lax.ppermute(right, "sub", [(i, i + 1) for i in range(subs - 1)])
    from_right = lax.ppermute(left, "sub", [(i + 1, i) for i in range(subs - 1)])
    return finish(tile_ids, base, from_left, from_right)


def solution(mesh):
    return jax.shard_map(
        shards,
        mesh=mesh,
        in_specs=(
            P("sub", "row", None, None, None),
            P("sub", "row", None, None),
            P("sub", "row", None),
            P("sub", "row", None),
            P("sub", None, "row", None),
            P(),
        ),
        out_specs=P("sub", None, "row", None),
        check_vma=False,
    )
```

```python
import functools

import jax
import jax.numpy as jnp
from jax import lax
from jax.experimental import pallas as pl
from jax.experimental.pallas import tpu as pltpu
from jax.sharding import PartitionSpec as P


F32 = jnp.float32
BF16 = jnp.bfloat16
VMEM_LIMIT = 24 * 1024 * 1024
ALONE = 63 * 1024 * 1024
SLOTS = 2
LAST = 4


def split(x):
    high = x.astype(BF16)
    return high, (x - high.astype(F32)).astype(BF16)


def nt(a, b):
    return lax.dot_general(a, b, (((1,), (1,)), ((), ())), preferred_element_type=F32)


def nn(a, b):
    return lax.dot_general(a, b, (((1,), (0,)), ((), ())), preferred_element_type=F32)


def three(dot, both, high, low):
    rows = both.shape[0] // 2
    wide = dot(both, high)
    return wide[:rows] + (wide[rows:] + dot(both[:rows], low))


def stacked(x):
    return jnp.concatenate(split(x), axis=0)


def substitute(off_ref, f, inverse, kept, acc, begin, finish):
    brows, kband = f.shape[0], f.shape[1]
    for i in range(brows):
        begin(i)
        for band in range(kband):
            source = i - off_ref[band, 0, i]
            if i > 0:

                @pl.when(source >= 0)
                def _():
                    acc[...] -= three(nt, kept[jnp.maximum(source, 0)], *split(f[i, band]))

        x = three(nt, stacked(acc[...]), *split(inverse[i]))
        if i + 1 < brows:
            kept[i] = stacked(x)
        finish(i, x)


def solve_kernel(off_ref, f_hbm, inv_hbm, b_hbm, *rest, first, chunks):
    outs, (f, inverse, b, kept, acc, sems) = rest[: len(chunks)], rest[len(chunks) :]
    brows, _, size, _ = f.shape
    total = sum(chunks)
    copies = []
    for i in range(brows):
        group = [
            pltpu.make_async_copy(inv_hbm.at[0, i], inverse.at[i], sems.at[0, i]),
            pltpu.make_async_copy(
                b_hbm.at[0, pl.ds(i * size, size), pl.ds(first, total)], b.at[i], sems.at[1, i]
            ),
        ]
        if i > 0:
            group.append(pltpu.make_async_copy(f_hbm.at[0, i], f.at[i], sems.at[2, i]))
        for copy in group:
            copy.start()
        copies.append(group)

    def begin(i):
        for copy in copies[i]:
            copy.wait()
        acc[...] = b[i].T

    def finish(i, x):
        start = 0
        for out, n in zip(outs, chunks):
            out[:, i * size : (i + 1) * size] = x[start : start + n]
            start += n

    substitute(off_ref, f, inverse, kept, acc, begin, finish)


def solve(offsets, blocks, inverses, coupling, first, chunks, limit):
    _, brows, kband, size, _ = blocks.shape
    total = sum(chunks)
    hbm = pl.BlockSpec(memory_space=pltpu.HBM)
    return pl.pallas_call(
        functools.partial(solve_kernel, first=first, chunks=chunks),
        in_specs=[pl.BlockSpec(memory_space=pltpu.SMEM), hbm, hbm, hbm],
        out_shape=[jax.ShapeDtypeStruct((n, brows * size), F32) for n in chunks],
        scratch_shapes=[
            pltpu.VMEM((brows, kband, size, size), F32),
            pltpu.VMEM((brows, size, size), F32),
            pltpu.VMEM((brows, size, total), F32),
            pltpu.VMEM((brows, 2 * total, size), BF16),
            pltpu.VMEM((total, size), F32),
            pltpu.SemaphoreType.DMA((3, brows)),
        ],
        compiler_params=pltpu.CompilerParams(vmem_limit_bytes=limit),
        cost_estimate=pl.CostEstimate(flops=6 * 10 * size * size * total, bytes_accessed=8 << 20, transcendentals=0),
    )(offsets, blocks, inverses, coupling)


def response_kernel(off_ref, f_hbm, inv_hbm, gh_ref, gl_ref, f, inverse, kept, acc, sems):
    brows, kband, size, _ = f.shape

    @pl.when(lax.axis_index("row") > 0)
    def _():
        copies = []
        for i in range(brows):
            group = [
                pltpu.make_async_copy(inv_hbm.at[0, i], inverse.at[i], sems.at[0, i]),
                pltpu.make_async_copy(f_hbm.at[0, i], f.at[i], sems.at[1, i]),
            ]
            for copy in group:
                copy.start()
            copies.append(group)

        def begin(i):
            for copy in copies[i]:
                copy.wait()
            acc[...] = jnp.zeros_like(acc)
            for band in range(kband):
                source = i - off_ref[band, 0, i]

                @pl.when(source < 0)
                def _():
                    at = pl.multiple_of((source + brows) * size, size)
                    acc[pl.ds(at, size), :] += f[i, band].T

        def finish(i, x):
            at = slice(i * size, (i + 1) * size)
            gh_ref[:, at], gl_ref[:, at] = split(x)

        substitute(off_ref, f, inverse, kept, acc, begin, finish)


def response(offsets, blocks, inverses):
    _, brows, kband, size, _ = blocks.shape
    width = brows * size
    hbm = pl.BlockSpec(memory_space=pltpu.HBM)
    return pl.pallas_call(
        response_kernel,
        in_specs=[pl.BlockSpec(memory_space=pltpu.SMEM), hbm, hbm],
        out_shape=[jax.ShapeDtypeStruct((width, width), BF16)] * 2,
        scratch_shapes=[
            pltpu.VMEM((brows, kband, size, size), F32),
            pltpu.VMEM((brows, size, size), F32),
            pltpu.VMEM((brows, 2 * width, size), BF16),
            pltpu.VMEM((width, size), F32),
            pltpu.SemaphoreType.DMA((2, brows)),
        ],
        compiler_params=pltpu.CompilerParams(vmem_limit_bytes=VMEM_LIMIT),
        cost_estimate=pl.CostEstimate(flops=6 * 10 * size * size * width, bytes_accessed=8 << 20, transcendentals=0),
        name="response",
    )(offsets, blocks, inverses)


def update_kernel(recv_ref, y_ref, cur_ref, gh_ref, gl_ref, out_ref, *, stage):
    out_ref[...] = cur_ref[...]

    @pl.when(lax.axis_index("row") == stage)
    def _():
        out_ref[...] = y_ref[...] - three(nn, stacked(recv_ref[...]), gh_ref[...], gl_ref[...])


def update(recv, y, cur, gain, stage):
    return pl.pallas_call(
        functools.partial(update_kernel, stage=stage),
        out_shape=jax.ShapeDtypeStruct(y.shape, F32),
        compiler_params=pltpu.CompilerParams(vmem_limit_bytes=VMEM_LIMIT),
        name="update",
    )(recv, y, cur, *gain)


def gram_kernel(*refs, start, fused, clear, last):
    recv_ref, y_ref = refs[:2]
    refs = refs[2:]
    if fused:
        gh_ref, gl_ref = refs[:2]
        refs = refs[2:]
    if start:
        oldh_ref, oldl_ref = refs[:2]
        refs = refs[2:]
    piece = refs[0]
    n, _ = recv_ref.shape
    here = slice(start, start + n)

    @pl.when(lax.axis_index("row") > 0)
    def _():
        recv = stacked(recv_ref[...])
        x = y_ref[...]
        if fused:
            x = x - three(nn, recv, gh_ref[...], gl_ref[...])
        x = stacked(x)
        high = jnp.concatenate([recv[:n], x[:n]], axis=1)
        low = jnp.concatenate([recv[n:], x[n:]], axis=1)
        both = jnp.concatenate([high, low], axis=0)
        if start:
            piece[:, :start] = three(nn, both, oldh_ref[:, :start], oldl_ref[:, :start])
        piece[:, here] = three(nt, both, high, low)
        if not last:
            refs[1][:, here] = high.T
            refs[2][:, here] = low.T

    if clear:

        @pl.when(lax.axis_index("row") == 0)
        def _():
            piece[...] = jnp.zeros_like(piece)


def gram(recv, y, gain, kept, start, total, clear):
    n, half = y.shape
    last = start + n == total
    fused = bool(gain)
    vmem = pl.BlockSpec(memory_space=pltpu.VMEM)
    inputs = [recv, y, *gain, *kept]
    results = pl.pallas_call(
        functools.partial(gram_kernel, start=start, fused=fused, clear=clear, last=last),
        in_specs=[vmem] * len(inputs),
        out_shape=[jax.ShapeDtypeStruct((n, start + n), F32)]
        + ([] if last else [jax.ShapeDtypeStruct((2 * half, total), BF16)] * 2),
        input_output_aliases={len(inputs) - 2 + i: 1 + i for i in range(2)} if start and not last else {},
        compiler_params=pltpu.CompilerParams(vmem_limit_bytes=VMEM_LIMIT),
        cost_estimate=pl.CostEstimate(
            flops=6 * n * half * (half + 2 * (start + n)), bytes_accessed=4 << 20, transcendentals=0
        ),
    )(*inputs)
    return results[0], list(results[1:])


def shared_slots(ids, mine, other, count):
    total = ids.shape[1]
    inside = jnp.logical_and(
        jnp.logical_and(mine >= 0, mine < total), jnp.logical_and(other >= 0, other < total)
    )
    mine, other = jnp.clip(mine, 0, total - 1), jnp.clip(other, 0, total - 1)
    found = jnp.int32(0)
    slots = [[jnp.int32(0), jnp.int32(0), jnp.bool_(False)] for _ in range(SLOTS)]
    for k in range(count):
        hit, place = jnp.bool_(False), jnp.int32(0)
        for i in range(count):
            same = ids[k, mine] == ids[i, other]
            hit = jnp.logical_or(hit, same)
            place = jnp.where(same, jnp.int32(i), place)
        hit = jnp.logical_and(hit, inside)
        for m, slot in enumerate(slots):
            take = jnp.logical_and(hit, found == m)
            slot[0] = jnp.where(take, jnp.int32(k), slot[0])
            slot[1] = jnp.where(take, place, slot[1])
            slot[2] = jnp.logical_or(slot[2], take)
        found = found + hit.astype(jnp.int32)
    return slots


def collect_kernel(ids_ref, face_ref, *refs, count, chunks, parts, exchanged):
    pieces, (base_ref, left_ref, right_ref, g) = refs[:-4], refs[-4:]
    _, share, cols = g.shape
    tile = cols // count
    row, sub = lax.axis_index("row"), lax.axis_index("sub")

    def fill(part):
        mine = pieces[len(chunks) :] if exchanged and part else pieces[: len(chunks)]
        low, high = part * share, (part + 1) * share
        start = 0
        for n, piece in zip(chunks, mine):
            at, inner = start // tile, start % tile
            first, stop = max(inner, low), min(inner + n, high)
            if first < stop:
                g[at, first - low : stop - low, : start + n] = piece[first - inner : stop - inner]
            turned = piece[:, :start].T if start else None
            for t in range(-(-start // tile)):
                stop = min(t * tile + high, start)
                first = t * tile + low
                if first < stop:
                    g[t, : stop - first, start : start + n] = turned[first:stop]
            start += n

    for part in range(parts):
        pl.when(row == part)(functools.partial(fill, part))
    base_ref[...] = face_ref[0] - g[...]
    for delta, out in ((-1, left_ref), (1, right_ref)):
        slots = shared_slots(ids_ref, sub, sub + delta, count)
        for m in range(SLOTS):
            for n in range(SLOTS):
                at = pl.multiple_of(slots[n][0] * tile, tile)
                out[m, :, n * tile : (n + 1) * tile] = g[slots[m][0], :, pl.ds(at, tile)]


def collect(ids, face, pieces, chunks, parts, exchanged):
    _, count, share, cols = face.shape
    smem = pl.BlockSpec(memory_space=pltpu.SMEM)
    vmem = pl.BlockSpec(memory_space=pltpu.VMEM)
    halo = jax.ShapeDtypeStruct((SLOTS, share, SLOTS * (cols // count)), F32)
    return pl.pallas_call(
        functools.partial(collect_kernel, count=count, chunks=chunks, parts=parts, exchanged=exchanged),
        in_specs=[smem, vmem] + [vmem] * len(pieces),
        out_shape=[jax.ShapeDtypeStruct((count, share, cols), F32), halo, halo],
        scratch_shapes=[pltpu.VMEM((count, share, cols), F32)],
        compiler_params=pltpu.CompilerParams(vmem_limit_bytes=VMEM_LIMIT),
        name="collect",
    )(ids, face, *pieces)


def finish_kernel(ids_ref, base_ref, left_ref, right_ref, out_ref, *, count):
    cols = base_ref.shape[2]
    tile = cols // count
    sub = lax.axis_index("sub")
    out_ref[0] = base_ref[...]
    for delta, halo in ((-1, left_ref), (1, right_ref)):
        slots = shared_slots(ids_ref, sub + delta, sub, count)
        for m in range(SLOTS):
            for n in range(SLOTS):

                @pl.when(jnp.logical_and(slots[m][2], slots[n][2]))
                def _():
                    at = pl.multiple_of(slots[n][1] * tile, tile)
                    out_ref[0, slots[m][1], :, pl.ds(at, tile)] -= halo[m, :, n * tile : (n + 1) * tile]


def finish(ids, base, left, right):
    count, share, cols = base.shape
    smem = pl.BlockSpec(memory_space=pltpu.SMEM)
    vmem = pl.BlockSpec(memory_space=pltpu.VMEM)
    return pl.pallas_call(
        functools.partial(finish_kernel, count=count),
        in_specs=[smem, vmem, vmem, vmem],
        out_shape=jax.ShapeDtypeStruct((1, count, share, cols), F32),
        compiler_params=pltpu.CompilerParams(vmem_limit_bytes=VMEM_LIMIT),
        name="finish",
    )(ids, base, left, right)


def sizes(count, tile):
    short = tile // LAST
    return (tile,) * (count - 1) + (tile - short, short)


def shards(factor_blocks, block_inverses, band_offsets, coupling, interface_block, tile_ids):
    rows = lax.axis_size("row")
    subs = lax.axis_size("sub")
    count = interface_block.shape[1]
    cols = coupling.shape[2]
    chunks = sizes(count, cols // count)
    offsets = jnp.transpose(band_offsets, (2, 0, 1))
    ids = jnp.transpose(tile_ids)
    ys = solve(offsets, factor_blocks, block_inverses, coupling, 0, chunks[:1], ALONE)
    ys += solve(offsets, factor_blocks, block_inverses, coupling, chunks[0], chunks[1:], VMEM_LIMIT)
    gain = response(offsets, factor_blocks, block_inverses)
    xs, first, gain_now = list(ys), None, gain if rows == 2 else ()
    for stage in range(1, rows):
        recv = []
        for x in xs:
            recv.append(lax.ppermute(x, "row", [(stage - 1, stage)]))
        first = first or recv
        if rows > 2:
            xs = [update(r, y, x, gain, stage) for r, y, x in zip(recv, ys, xs)]
    kept, own, got, start = [], [], [], 0
    for c, n in enumerate(chunks):
        piece, kept = gram(first[c], xs[c], gain_now, kept, start, cols, rows > 2)
        start += n
        if rows == 2:
            got.append(lax.ppermute(piece, "row", [(1, 0)]))
            own.append(piece)
        else:
            got.append(lax.psum(piece, "row"))
    base, left, right = collect(ids, interface_block, got + own, chunks, rows, rows == 2)
    from_left = lax.ppermute(right, "sub", [(i, i + 1) for i in range(subs - 1)])
    from_right = lax.ppermute(left, "sub", [(i + 1, i) for i in range(subs - 1)])
    return finish(ids, base, from_left, from_right)


def solution(mesh):
    return jax.shard_map(
        shards,
        mesh=mesh,
        in_specs=(
            P("sub", "row", None, None, None),
            P("sub", "row", None, None),
            P("sub", "row", None),
            P("sub", "row", None),
            P("sub", None, "row", None),
            P(),
        ),
        out_specs=P("sub", None, "row", None),
        check_vma=False,
    )
```

```python
import functools

import jax
import jax.numpy as jnp
from jax import lax
from jax.experimental import pallas as pl
from jax.experimental.pallas import tpu as pltpu
from jax.sharding import PartitionSpec as P


F32 = jnp.float32
BF16 = jnp.bfloat16
VMEM_LIMIT = 24 * 1024 * 1024
ALONE = 63 * 1024 * 1024
PAIR = 2
LAST = 4


def split(x):
    high = x.astype(BF16)
    return high, (x - high.astype(F32)).astype(BF16)


def nt(a, b):
    return lax.dot_general(a, b, (((1,), (1,)), ((), ())), preferred_element_type=F32)


def nn(a, b):
    return lax.dot_general(a, b, (((1,), (0,)), ((), ())), preferred_element_type=F32)


def three(dot, both, high, low):
    rows = both.shape[0] // 2
    wide = dot(both, high)
    return wide[:rows] + (wide[rows:] + dot(both[:rows], low))


def stacked(x):
    return jnp.concatenate(split(x), axis=0)


def near_of(sub):
    return sub + 1 - 2 * (sub % 2)


def far_of(sub):
    return sub - 1 + 2 * (sub % 2)


def shares(ids, k, sub, other):
    count, total = ids.shape
    inside = jnp.logical_and(other >= 0, other < total)
    other = jnp.clip(other, 0, total - 1)
    hit = ids[k, sub] == ids[0, other]
    for i in range(1, count):
        hit = jnp.logical_or(hit, ids[k, sub] == ids[i, other])
    return jnp.logical_and(hit, inside)


def ordered(ids, sub):
    count = ids.shape[0]
    keys = []
    for k in range(count):
        far = shares(ids, k, sub, far_of(sub)).astype(jnp.int32)
        near = shares(ids, k, sub, near_of(sub)).astype(jnp.int32)
        keys.append((1 + near - far) * count + k)
    order = [jnp.int32(0)] * count
    for k in range(count):
        place = sum((keys[j] < keys[k]).astype(jnp.int32) for j in range(count) if j != k)
        order = [jnp.where(place == p, jnp.int32(k), order[p]) for p in range(count)]
    return order


def wait_all(copies):
    for copy in copies:
        copy.wait()


def substitute(off_ref, f, inverse, begin, finish):
    brows, kband = f.shape[0], f.shape[1]
    solved = []
    for i in range(brows):
        rest = begin(i)
        for j in range(i):
            at, found = jnp.int32(0), jnp.bool_(False)
            for band in range(kband):
                same = off_ref[band, 0, i] == i - j
                at = jnp.where(same, jnp.int32(band), at)
                found = jnp.logical_or(found, same)
            block = jnp.where(found, f[i, at], 0.0)
            rest = rest - three(nt, solved[j], *split(block))
        x = three(nt, stacked(rest), *split(inverse[i]))
        solved.append(stacked(x))
        finish(i, x)


def solve_kernel(off_ref, ids_ref, f_hbm, inv_hbm, b_hbm, *rest, chunks, tiles, first_only):
    outs, (f, inverse, b, sems) = rest[: len(chunks)], rest[len(chunks) :]
    brows, _, size, _ = f.shape
    tile = b.shape[2] // tiles

    def run():
        order = ordered(ids_ref, lax.axis_index("sub"))
        copies = []
        for i in range(brows):
            group = [pltpu.make_async_copy(inv_hbm.at[0, i], inverse.at[i], sems.at[0, i])]
            for p in range(tiles):
                columns = pl.ds(pl.multiple_of(order[p] * tile, tile), tile)
                group.append(
                    pltpu.make_async_copy(
                        b_hbm.at[0, pl.ds(i * size, size), columns],
                        b.at[i, :, pl.ds(p * tile, tile)],
                        sems.at[2 + p, i],
                    )
                )
            if i > 0:
                group.append(pltpu.make_async_copy(f_hbm.at[0, i], f.at[i], sems.at[1, i]))
            for copy in group:
                copy.start()
            copies.append(group)

        def begin(i):
            wait_all(copies[i])
            return b[i].T

        def finish(i, x):
            start = 0
            for out, n in zip(outs, chunks):
                out[:, i * size : (i + 1) * size] = x[start : start + n]
                start += n

        substitute(off_ref, f, inverse, begin, finish)

    if first_only:
        pl.when(lax.axis_index("row") == 0)(run)
    else:
        run()


def solve(offsets, ids, blocks, inverses, coupling, chunks, tile, first_only, limit):
    _, brows, kband, size, _ = blocks.shape
    total = sum(chunks)
    tiles = total // tile
    hbm = pl.BlockSpec(memory_space=pltpu.HBM)
    smem = pl.BlockSpec(memory_space=pltpu.SMEM)
    return pl.pallas_call(
        functools.partial(solve_kernel, chunks=chunks, tiles=tiles, first_only=first_only),
        in_specs=[smem, smem, hbm, hbm, hbm],
        out_shape=[jax.ShapeDtypeStruct((n, brows * size), F32) for n in chunks],
        scratch_shapes=[
            pltpu.VMEM((brows, kband, size, size), F32),
            pltpu.VMEM((brows, size, size), F32),
            pltpu.VMEM((brows, size, total), F32),
            pltpu.SemaphoreType.DMA((2 + tiles, brows)),
        ],
        compiler_params=pltpu.CompilerParams(vmem_limit_bytes=limit),
        cost_estimate=pl.CostEstimate(flops=6 * 10 * size * size * total, bytes_accessed=8 << 20, transcendentals=0),
    )(offsets, ids, blocks, inverses, coupling)


def response_kernel(off_ref, f_hbm, inv_hbm, gh_ref, gl_ref, f, inverse, acc, sems):
    brows, kband, size, _ = f.shape

    @pl.when(lax.axis_index("row") > 0)
    def _():
        copies = []
        for i in range(brows):
            group = [
                pltpu.make_async_copy(inv_hbm.at[0, i], inverse.at[i], sems.at[0, i]),
                pltpu.make_async_copy(f_hbm.at[0, i], f.at[i], sems.at[1, i]),
            ]
            for copy in group:
                copy.start()
            copies.append(group)

        def begin(i):
            wait_all(copies[i])
            acc[...] = jnp.zeros_like(acc)
            for band in range(kband):
                source = i - off_ref[band, 0, i]

                @pl.when(source < 0)
                def _():
                    at = pl.multiple_of((source + brows) * size, size)
                    acc[pl.ds(at, size), :] += f[i, band].T

            return acc[...]

        def finish(i, x):
            at = slice(i * size, (i + 1) * size)
            gh_ref[:, at], gl_ref[:, at] = split(x)

        substitute(off_ref, f, inverse, begin, finish)


def response(offsets, blocks, inverses):
    _, brows, kband, size, _ = blocks.shape
    width = brows * size
    hbm = pl.BlockSpec(memory_space=pltpu.HBM)
    return pl.pallas_call(
        response_kernel,
        in_specs=[pl.BlockSpec(memory_space=pltpu.SMEM), hbm, hbm],
        out_shape=[jax.ShapeDtypeStruct((width, width), BF16)] * 2,
        scratch_shapes=[
            pltpu.VMEM((brows, kband, size, size), F32),
            pltpu.VMEM((brows, size, size), F32),
            pltpu.VMEM((width, size), F32),
            pltpu.SemaphoreType.DMA((2, brows)),
        ],
        compiler_params=pltpu.CompilerParams(vmem_limit_bytes=VMEM_LIMIT),
        cost_estimate=pl.CostEstimate(flops=6 * 10 * size * size * width, bytes_accessed=8 << 20, transcendentals=0),
        name="response",
    )(offsets, blocks, inverses)


def update_kernel(recv_ref, y_ref, cur_ref, gh_ref, gl_ref, out_ref, *, stage):
    out_ref[...] = cur_ref[...]

    @pl.when(lax.axis_index("row") == stage)
    def _():
        out_ref[...] = y_ref[...] - three(nn, stacked(recv_ref[...]), gh_ref[...], gl_ref[...])


def update(recv, y, cur, gain, stage):
    return pl.pallas_call(
        functools.partial(update_kernel, stage=stage),
        out_shape=jax.ShapeDtypeStruct(y.shape, F32),
        compiler_params=pltpu.CompilerParams(vmem_limit_bytes=VMEM_LIMIT),
        name="update",
    )(recv, y, cur, *gain)


def gram_kernel(*refs, start, fused, clear, last):
    recv_ref, y_ref = refs[:2]
    refs = refs[2:]
    if fused:
        gh_ref, gl_ref = refs[:2]
        refs = refs[2:]
    if start:
        oldh_ref, oldl_ref = refs[:2]
        refs = refs[2:]
    piece = refs[0]
    n, _ = recv_ref.shape
    here = slice(start, start + n)

    @pl.when(lax.axis_index("row") > 0)
    def _():
        recv = stacked(recv_ref[...])
        x = y_ref[...]
        if fused:
            x = x - three(nn, recv, gh_ref[...], gl_ref[...])
        x = stacked(x)
        high = jnp.concatenate([recv[:n], x[:n]], axis=1)
        low = jnp.concatenate([recv[n:], x[n:]], axis=1)
        both = jnp.concatenate([high, low], axis=0)
        if start:
            piece[:, :start] = three(nn, both, oldh_ref[:, :start], oldl_ref[:, :start])
        piece[:, here] = three(nt, both, high, low)
        if not last:
            refs[1][:, here] = high.T
            refs[2][:, here] = low.T

    if clear:

        @pl.when(lax.axis_index("row") == 0)
        def _():
            piece[...] = jnp.zeros_like(piece)


def gram(recv, y, gain, kept, start, total, clear):
    n, half = y.shape
    last = start + n == total
    fused = bool(gain)
    vmem = pl.BlockSpec(memory_space=pltpu.VMEM)
    inputs = [recv, y, *gain, *kept]
    results = pl.pallas_call(
        functools.partial(gram_kernel, start=start, fused=fused, clear=clear, last=last),
        in_specs=[vmem] * len(inputs),
        out_shape=[jax.ShapeDtypeStruct((n, start + n), F32)]
        + ([] if last else [jax.ShapeDtypeStruct((2 * half, total), BF16)] * 2),
        input_output_aliases={len(inputs) - 2 + i: 1 + i for i in range(2)} if start and not last else {},
        compiler_params=pltpu.CompilerParams(vmem_limit_bytes=VMEM_LIMIT),
        cost_estimate=pl.CostEstimate(
            flops=6 * n * half * (half + 2 * (start + n)), bytes_accessed=4 << 20, transcendentals=0
        ),
    )(*inputs)
    return results[0], list(results[1:])


def fill(out, chunks, part, tile, low_tile):
    share = out.shape[1]
    low, high = part * share, (part + 1) * share
    base = low_tile * tile
    for start, piece in chunks:
        n = piece.shape[0]
        at, inner = start // tile, start % tile
        first, stop = max(inner, low), min(inner + n, high)
        if first < stop:
            out[at - low_tile, first - low : stop - low, : start + n - base] = piece[first - inner : stop - inner, base:]
        if start > base:
            turned = piece[:, base:start].T
            for t in range(low_tile, -(-start // tile)):
                first, stop = t * tile + low, min(t * tile + high, start)
                if first < stop:
                    out[t - low_tile, : stop - first, start - base : start - base + n] = turned[
                        first - base : stop - base
                    ]


def fill_mine(out, starts, pieces, parts, tile, low_tile):
    row = lax.axis_index("row")
    both = len(pieces) > len(starts)
    for part in range(parts):
        mine = pieces[len(starts) :] if both and part else pieces[: len(starts)]
        pl.when(row == part)(functools.partial(fill, out, list(zip(starts, mine)), part, tile, low_tile))


def pair_kernel(*refs, starts, parts, tile, low_tile):
    fill_mine(refs[-1], starts, refs[:-1], parts, tile, low_tile)


def pair(pieces, starts, parts, tile, share, low_tile):
    return pl.pallas_call(
        functools.partial(pair_kernel, starts=starts, parts=parts, tile=tile, low_tile=low_tile),
        out_shape=jax.ShapeDtypeStruct((PAIR, share, PAIR * tile), F32),
        compiler_params=pltpu.CompilerParams(vmem_limit_bytes=VMEM_LIMIT),
    )(*pieces)


def subtract_halo(ids, out, halo, other, low_tile):
    count, total = ids.shape
    tile = halo.shape[2] // PAIR
    sub = lax.axis_index("sub")
    inside = jnp.logical_and(other >= 0, other < total)
    other = jnp.clip(other, 0, total - 1)
    order = ordered(ids, other)
    slots = []
    for m in range(PAIR):
        number = ids[order[low_tile + m], other]
        place, hit = jnp.int32(0), jnp.bool_(False)
        for i in range(count):
            same = ids[i, sub] == number
            place = jnp.where(same, jnp.int32(i), place)
            hit = jnp.logical_or(hit, same)
        slots.append((place, jnp.logical_and(hit, inside)))
    for m in range(PAIR):
        for n in range(PAIR):

            @pl.when(jnp.logical_and(slots[m][1], slots[n][1]))
            def _():
                at = pl.multiple_of(slots[n][0] * tile, tile)
                out[slots[m][0], :, pl.ds(at, tile)] -= halo[m, :, n * tile : (n + 1) * tile]


def middle_kernel(ids_ref, face_ref, halo_ref, *refs, starts, parts, tile):
    pieces, (out_ref, g) = refs[:-2], refs[-2:]
    fill_mine(g, starts, pieces, parts, tile, 0)
    out_ref[...] = face_ref[0]
    sub = lax.axis_index("sub")
    order = ordered(ids_ref, sub)
    for p in range(PAIR):
        for q in range(PAIR):
            at = pl.multiple_of(order[q] * tile, tile)
            out_ref[order[p], :, pl.ds(at, tile)] -= g[p, :, q * tile : (q + 1) * tile]
    subtract_halo(ids_ref, out_ref, halo_ref, far_of(sub), 0)


def rest_kernel(ids_ref, base_ref, *refs, starts, parts, tile):
    pieces, (out_ref, g) = refs[:-2], refs[-2:]
    count = base_ref.shape[0]
    fill_mine(g, starts, pieces, parts, tile, 0)
    out_ref[...] = base_ref[...]
    order = ordered(ids_ref, lax.axis_index("sub"))
    for p in range(count):
        for q in range(count):
            if p >= PAIR or q >= PAIR:
                at = pl.multiple_of(order[q] * tile, tile)
                out_ref[order[p], :, pl.ds(at, tile)] -= g[p, :, q * tile : (q + 1) * tile]


def finish_kernel(ids_ref, base_ref, halo_ref, out_ref, *, low_tile):
    out_ref[...] = base_ref[...]
    subtract_halo(ids_ref, out_ref, halo_ref, near_of(lax.axis_index("sub")), low_tile)


def assemble(kernel, ids, arrays, shape, scratch):
    smem = pl.BlockSpec(memory_space=pltpu.SMEM)
    vmem = pl.BlockSpec(memory_space=pltpu.VMEM)
    return pl.pallas_call(
        kernel,
        in_specs=[smem] + [vmem] * len(arrays),
        out_shape=jax.ShapeDtypeStruct(shape, F32),
        scratch_shapes=[pltpu.VMEM(scratch, F32)] if scratch else [],
        compiler_params=pltpu.CompilerParams(vmem_limit_bytes=VMEM_LIMIT),
    )(ids, *arrays)


def sizes(count, tile):
    short = tile // LAST
    return (tile,) * (count - 1) + (tile - short, short)


def shards(factor_blocks, block_inverses, band_offsets, coupling, interface_block, tile_ids):
    rows = lax.axis_size("row")
    subs = lax.axis_size("sub")
    _, count, share, cols = interface_block.shape
    tile = cols // count
    chunks = sizes(count, tile)
    starts = [sum(chunks[:c]) for c in range(len(chunks))]
    offsets = jnp.transpose(band_offsets, (2, 0, 1))
    ids = jnp.transpose(tile_ids)
    given = (offsets, ids, factor_blocks, block_inverses, coupling)
    far = [(s, s - 1 + 2 * (s % 2)) for s in range(subs)]
    near = [(s, s + 1 - 2 * (s % 2)) for s in range(subs)]
    far, near = ([(s, t) for s, t in pairs if 0 <= t < subs] for pairs in (far, near))
    early = solve(*given, chunks[:1], tile, True, ALONE)
    ys = solve(*given, chunks, tile, False, VMEM_LIMIT)
    gain = response(offsets, factor_blocks, block_inverses)
    xs, first, gain_now = early + ys[1:], None, gain if rows == 2 else ()
    for stage in range(1, rows):
        recv = []
        for x in xs:
            recv.append(lax.ppermute(x, "row", [(stage - 1, stage)]))
        first = first or recv
        if rows > 2:
            xs = [update(r, y, x, gain, stage) for r, y, x in zip(recv, ys, xs)]
    kept, own, got = [], [], []
    for c, start in enumerate(starts):
        piece, kept = gram(first[c], (ys if rows == 2 else xs)[c], gain_now, kept, start, cols, rows > 2)
        if rows == 2:
            got.append(lax.ppermute(piece, "row", [(1, 0)]))
            own.append(piece)
        else:
            got.append(lax.psum(piece, "row"))
    shape = (count, share, cols)
    last = count - PAIR

    def pick(low, high):
        return got[low:high] + own[low:high]

    message = pair(pick(0, PAIR), starts[:PAIR], rows, tile, share, 0)
    from_far = lax.ppermute(message, "sub", far)
    kernel = functools.partial(middle_kernel, starts=starts[:PAIR], parts=rows, tile=tile)
    base = assemble(kernel, ids, [interface_block, from_far] + pick(0, PAIR), shape, (PAIR, share, PAIR * tile))
    message = pair(pick(last, None), starts[last:], rows, tile, share, last)
    from_near = lax.ppermute(message, "sub", near)
    kernel = functools.partial(rest_kernel, starts=starts[PAIR:], parts=rows, tile=tile)
    base = assemble(kernel, ids, [base] + pick(PAIR, None), shape, shape)
    kernel = functools.partial(finish_kernel, low_tile=last)
    return assemble(kernel, ids, [base, from_near], shape, None)[None]


def solution(mesh):
    return jax.shard_map(
        shards,
        mesh=mesh,
        in_specs=(
            P("sub", "row", None, None, None),
            P("sub", "row", None, None),
            P("sub", "row", None),
            P("sub", "row", None),
            P("sub", None, "row", None),
            P(),
        ),
        out_specs=P("sub", None, "row", None),
        check_vma=False,
    )
```

```python
import functools

import jax
import jax.numpy as jnp
from jax import lax
from jax.experimental import pallas as pl
from jax.experimental.pallas import tpu as pltpu
from jax.sharding import PartitionSpec as P


F32 = jnp.float32
BF16 = jnp.bfloat16
VMEM_LIMIT = 24 * 1024 * 1024
OTHERS = 24 * 1024 * 1024
ALONE = 63 * 1024 * 1024
PAIR = 2
LAST = (3, 8)


def split(x):
    high = x.astype(BF16)
    return high, (x - high.astype(F32)).astype(BF16)


def nt(a, b):
    return lax.dot_general(a, b, (((1,), (1,)), ((), ())), preferred_element_type=F32)


def nn(a, b):
    return lax.dot_general(a, b, (((1,), (0,)), ((), ())), preferred_element_type=F32)


def three(dot, both, high, low):
    rows = both.shape[0] // 2
    wide = dot(both, high)
    return wide[:rows] + (wide[rows:] + dot(both[:rows], low))


def stacked(x):
    return jnp.concatenate(split(x), axis=0)


def near_of(sub):
    return sub + 1 - 2 * (sub % 2)


def far_of(sub):
    return sub - 1 + 2 * (sub % 2)


def shares(ids, k, sub, other):
    count, total = ids.shape
    inside = jnp.logical_and(other >= 0, other < total)
    other = jnp.clip(other, 0, total - 1)
    hit = ids[k, sub] == ids[0, other]
    for i in range(1, count):
        hit = jnp.logical_or(hit, ids[k, sub] == ids[i, other])
    return jnp.logical_and(hit, inside)


def ordered(ids, sub):
    count = ids.shape[0]
    keys = []
    for k in range(count):
        far = shares(ids, k, sub, far_of(sub)).astype(jnp.int32)
        near = shares(ids, k, sub, near_of(sub)).astype(jnp.int32)
        keys.append((1 + near - far) * count + k)
    order = [jnp.int32(0)] * count
    for k in range(count):
        place = sum((keys[j] < keys[k]).astype(jnp.int32) for j in range(count) if j != k)
        order = [jnp.where(place == p, jnp.int32(k), order[p]) for p in range(count)]
    return order


def wait_all(copies):
    for copy in copies:
        copy.wait()


def substitute(off_ref, f, inverse, begin, finish):
    brows, kband = f.shape[0], f.shape[1]
    solved = []
    for i in range(brows):
        rest = begin(i)
        for j in range(i):
            at, found = jnp.int32(0), jnp.bool_(False)
            for band in range(kband):
                same = off_ref[band, 0, i] == i - j
                at = jnp.where(same, jnp.int32(band), at)
                found = jnp.logical_or(found, same)
            block = jnp.where(found, f[i, at], 0.0)
            rest = rest - three(nt, solved[j], *split(block))
        x = three(nt, stacked(rest), *split(inverse[i]))
        solved.append(stacked(x))
        finish(i, x)


def early_kernel(ids_hbm, inv_hbm, b_hbm, out, ids_ref, inverse, b, x_ref, sems):
    @pl.when(lax.axis_index("row") == 0)
    def _():
        size = inverse.shape[0]
        copies = [
            pltpu.make_async_copy(inv_hbm.at[0, 0], inverse, sems.at[0]),
            pltpu.make_async_copy(b_hbm.at[0, pl.ds(0, size)], b, sems.at[1]),
            pltpu.make_async_copy(ids_hbm, ids_ref, sems.at[2]),
        ]
        for copy in copies:
            copy.start()
        copies[1].wait()
        right = stacked(b[...].T)
        copies[0].wait()
        x_ref[...] = three(nt, right, *split(inverse[...]))
        copies[2].wait()
        order = ordered(ids_ref, lax.axis_index("sub"))
        tile = x_ref.shape[0] // len(order)
        for p, k in enumerate(order):
            out[p * tile : (p + 1) * tile] = x_ref[pl.ds(pl.multiple_of(k * tile, tile), tile)]


def early_solve(ids, inverses, coupling):
    size, cols = inverses.shape[2], coupling.shape[2]
    hbm = pl.BlockSpec(memory_space=pltpu.HBM)
    return pl.pallas_call(
        early_kernel,
        in_specs=[hbm] * 3,
        out_shape=jax.ShapeDtypeStruct((cols, size), F32),
        scratch_shapes=[
            pltpu.SMEM(ids.shape, jnp.int32),
            pltpu.VMEM((size, size), F32),
            pltpu.VMEM((size, cols), F32),
            pltpu.VMEM((cols, size), F32),
            pltpu.SemaphoreType.DMA((3,)),
        ],
        compiler_params=pltpu.CompilerParams(vmem_limit_bytes=ALONE),
        cost_estimate=pl.CostEstimate(flops=6 * size * size * cols, bytes_accessed=1 << 20, transcendentals=0),
        name="early",
    )(ids, inverses, coupling)


def solve_kernel(off_ref, ids_ref, f_hbm, inv_hbm, b_hbm, top, *rest, chunks, tiles):
    outs, (f, inverse, b, sems) = rest[: len(chunks)], rest[len(chunks) :]
    brows, _, size, _ = f.shape
    tile = b.shape[2] // tiles

    order = ordered(ids_ref, lax.axis_index("sub"))
    copies = []
    for i in range(brows):
        group = [pltpu.make_async_copy(inv_hbm.at[0, i], inverse.at[i], sems.at[0, i])]
        for p in range(tiles):
            columns = pl.ds(pl.multiple_of(order[p] * tile, tile), tile)
            group.append(
                pltpu.make_async_copy(
                    b_hbm.at[0, pl.ds(i * size, size), columns],
                    b.at[i, :, pl.ds(p * tile, tile)],
                    sems.at[2 + p, i],
                )
            )
        if i > 0:
            group.append(pltpu.make_async_copy(f_hbm.at[0, i], f.at[i], sems.at[1, i]))
        for copy in group:
            copy.start()
        copies.append(group)

    def begin(i):
        wait_all(copies[i])
        return b[i].T

    def finish(i, x):
        if i == 0:
            top[...] = x
            return
        start = 0
        for out, n in zip(outs, chunks):
            out[:, (i - 1) * size : i * size] = x[start : start + n]
            start += n

    substitute(off_ref, f, inverse, begin, finish)


def solve(offsets, ids, blocks, inverses, coupling, chunks, tile):
    _, brows, kband, size, _ = blocks.shape
    total = sum(chunks)
    tiles = total // tile
    hbm = pl.BlockSpec(memory_space=pltpu.HBM)
    smem = pl.BlockSpec(memory_space=pltpu.SMEM)
    return pl.pallas_call(
        functools.partial(solve_kernel, chunks=chunks, tiles=tiles),
        in_specs=[smem, smem, hbm, hbm, hbm],
        out_shape=[jax.ShapeDtypeStruct((total, size), F32)]
        + [jax.ShapeDtypeStruct((n, (brows - 1) * size), F32) for n in chunks],
        scratch_shapes=[
            pltpu.VMEM((brows, kband, size, size), F32),
            pltpu.VMEM((brows, size, size), F32),
            pltpu.VMEM((brows, size, total), F32),
            pltpu.SemaphoreType.DMA((2 + tiles, brows)),
        ],
        compiler_params=pltpu.CompilerParams(vmem_limit_bytes=OTHERS),
        cost_estimate=pl.CostEstimate(flops=6 * 10 * size * size * total, bytes_accessed=8 << 20, transcendentals=0),
        name="others",
    )(offsets, ids, blocks, inverses, coupling)


def response_kernel(off_ref, f_hbm, inv_hbm, gh_ref, gl_ref, f, inverse, acc, sems):
    brows, kband, size, _ = f.shape

    @pl.when(lax.axis_index("row") > 0)
    def _():
        copies = []
        for i in range(brows):
            group = [
                pltpu.make_async_copy(inv_hbm.at[0, i], inverse.at[i], sems.at[0, i]),
                pltpu.make_async_copy(f_hbm.at[0, i], f.at[i], sems.at[1, i]),
            ]
            for copy in group:
                copy.start()
            copies.append(group)

        def begin(i):
            wait_all(copies[i])
            acc[...] = jnp.zeros_like(acc)
            for band in range(kband):
                source = i - off_ref[band, 0, i]

                @pl.when(source < 0)
                def _():
                    at = pl.multiple_of((source + brows) * size, size)
                    acc[pl.ds(at, size), :] += f[i, band].T

            return acc[...]

        def finish(i, x):
            at = slice(i * size, (i + 1) * size)
            gh_ref[:, at], gl_ref[:, at] = split(x)

        substitute(off_ref, f, inverse, begin, finish)


def response(offsets, blocks, inverses):
    _, brows, kband, size, _ = blocks.shape
    width = brows * size
    hbm = pl.BlockSpec(memory_space=pltpu.HBM)
    return pl.pallas_call(
        response_kernel,
        in_specs=[pl.BlockSpec(memory_space=pltpu.SMEM), hbm, hbm],
        out_shape=[jax.ShapeDtypeStruct((width, width), BF16)] * 2,
        scratch_shapes=[
            pltpu.VMEM((brows, kband, size, size), F32),
            pltpu.VMEM((brows, size, size), F32),
            pltpu.VMEM((width, size), F32),
            pltpu.SemaphoreType.DMA((2, brows)),
        ],
        compiler_params=pltpu.CompilerParams(vmem_limit_bytes=VMEM_LIMIT),
        cost_estimate=pl.CostEstimate(flops=6 * 10 * size * size * width, bytes_accessed=8 << 20, transcendentals=0),
        name="response",
    )(offsets, blocks, inverses)


def update_kernel(*refs, chunks, stage):
    gh_ref, gl_ref = refs[:2]
    width = 1 + len(chunks)
    recv, y, cur, out = (refs[2 + k * width : 2 + (k + 1) * width] for k in range(4))
    for source, target in zip(cur, out):
        target[...] = source[...]

    @pl.when(lax.axis_index("row") == stage)
    def _():
        size = recv[0].shape[1]
        start = 0
        for c, n in enumerate(chunks):
            rows = slice(start, start + n)
            given = jnp.concatenate([recv[0][rows], recv[1 + c][...]], axis=1)
            change = three(nn, stacked(given), gh_ref[...], gl_ref[...])
            out[0][rows] = y[0][rows] - change[:, :size]
            out[1 + c][...] = y[1 + c][...] - change[:, size:]
            start += n


def update(recv, y, cur, gain, chunks, stage):
    return pl.pallas_call(
        functools.partial(update_kernel, chunks=chunks, stage=stage),
        out_shape=[jax.ShapeDtypeStruct(x.shape, F32) for x in y],
        compiler_params=pltpu.CompilerParams(vmem_limit_bytes=VMEM_LIMIT),
        name="update",
    )(*gain, *recv, *y, *cur)


def gram_kernel(*refs, start, fused, clear, last, share, tile):
    recv0_ref, recv_ref, y0_ref, y_ref = refs[:4]
    refs = refs[4:]
    if fused:
        gh_ref, gl_ref = refs[:2]
        refs = refs[2:]
    if start:
        oldh_ref, oldl_ref = refs[:2]
        refs = refs[2:]
    piece, rest = refs[0], refs[1:]
    n = recv_ref.shape[0]
    here = slice(start, start + n)

    @pl.when(lax.axis_index("row") > 0)
    def _():
        recv = stacked(jnp.concatenate([recv0_ref[here], recv_ref[...]], axis=1))
        x = jnp.concatenate([y0_ref[here], y_ref[...]], axis=1)
        if fused:
            x = x - three(nn, recv, gh_ref[...], gl_ref[...])
        x = stacked(x)
        high = jnp.concatenate([recv[:n], x[:n]], axis=1)
        low = jnp.concatenate([recv[n:], x[n:]], axis=1)
        both = jnp.concatenate([high, low], axis=0)
        if start:
            piece[:, :start] = three(nn, both, oldh_ref[:, :start], oldl_ref[:, :start])
        piece[:, here] = three(nt, both, high, low)
        if not last:
            rest[0][:, here] = high.T
            rest[1][:, here] = low.T
        elif share:
            rest[0][...] = jnp.concatenate(
                [piece[:, t * tile : t * tile + share] for t in range((start + n) // tile)], axis=1
            )

    if clear:

        @pl.when(lax.axis_index("row") == 0)
        def _():
            piece[...] = jnp.zeros_like(piece)


def gram(recv, y, gain, kept, start, total, tile, share, clear):
    n = recv[1].shape[0]
    half = recv[0].shape[1] + recv[1].shape[1]
    last = start + n == total
    inputs = [*recv, *y, *gain, *kept]
    if not last:
        more = [jax.ShapeDtypeStruct((2 * half, total), BF16)] * 2
    else:
        more = [jax.ShapeDtypeStruct((n, total // tile * share), F32)] if share else []
    results = pl.pallas_call(
        functools.partial(
            gram_kernel, start=start, fused=bool(gain), clear=clear, last=last, share=share, tile=tile
        ),
        in_specs=[pl.BlockSpec(memory_space=pltpu.VMEM)] * len(inputs),
        out_shape=[jax.ShapeDtypeStruct((n, start + n), F32)] + more,
        input_output_aliases={len(inputs) - 2 + i: 1 + i for i in range(2)} if start and not last else {},
        compiler_params=pltpu.CompilerParams(vmem_limit_bytes=VMEM_LIMIT),
        cost_estimate=pl.CostEstimate(
            flops=6 * n * half * (half + 2 * (start + n)), bytes_accessed=4 << 20, transcendentals=0
        ),
    )(*inputs)
    return results[0], list(results[1:])


def fill(out, chunks, part, tile, low_tile):
    share = out.shape[1]
    low, high = part * share, (part + 1) * share
    base = low_tile * tile
    for start, piece in chunks:
        n = piece.shape[0]
        at, inner = start // tile, start % tile
        if piece.shape[1] < start + n:
            turned = piece[:, low_tile * share :].T
            for t in range(low_tile, at + 1):
                first = (t - low_tile) * share
                out[t - low_tile, :, start - base : start - base + n] = turned[first : first + share]
            continue
        first, stop = max(inner, low), min(inner + n, high)
        if first < stop:
            out[at - low_tile, first - low : stop - low, : start + n - base] = piece[first - inner : stop - inner, base:]
        if start > base:
            turned = piece[:, base:start].T
            for t in range(low_tile, -(-start // tile)):
                first, stop = t * tile + low, min(t * tile + high, start)
                if first < stop:
                    out[t - low_tile, : stop - first, start - base : start - base + n] = turned[
                        first - base : stop - base
                    ]


def fill_mine(out, starts, pieces, parts, tile, low_tile):
    row = lax.axis_index("row")
    both = len(pieces) > len(starts)
    for part in range(parts):
        mine = pieces[len(starts) :] if both and part else pieces[: len(starts)]
        pl.when(row == part)(functools.partial(fill, out, list(zip(starts, mine)), part, tile, low_tile))


def pair_kernel(*refs, starts, parts, tile, low_tile):
    fill_mine(refs[-1], starts, refs[:-1], parts, tile, low_tile)


def pair(pieces, starts, parts, tile, share, low_tile):
    return pl.pallas_call(
        functools.partial(pair_kernel, starts=starts, parts=parts, tile=tile, low_tile=low_tile),
        out_shape=jax.ShapeDtypeStruct((PAIR, share, PAIR * tile), F32),
        compiler_params=pltpu.CompilerParams(vmem_limit_bytes=VMEM_LIMIT),
    )(*pieces)


def subtract_halo(ids, out, halo, other, low_tile):
    count, total = ids.shape
    tile = halo.shape[2] // PAIR
    sub = lax.axis_index("sub")
    inside = jnp.logical_and(other >= 0, other < total)
    other = jnp.clip(other, 0, total - 1)
    order = ordered(ids, other)
    slots = []
    for m in range(PAIR):
        number = ids[order[low_tile + m], other]
        place, hit = jnp.int32(0), jnp.bool_(False)
        for i in range(count):
            same = ids[i, sub] == number
            place = jnp.where(same, jnp.int32(i), place)
            hit = jnp.logical_or(hit, same)
        slots.append((place, jnp.logical_and(hit, inside)))
    for m in range(PAIR):
        for n in range(PAIR):

            @pl.when(jnp.logical_and(slots[m][1], slots[n][1]))
            def _():
                at = pl.multiple_of(slots[n][0] * tile, tile)
                out[slots[m][0], :, pl.ds(at, tile)] -= halo[m, :, n * tile : (n + 1) * tile]


def middle_kernel(ids_ref, face_ref, halo_ref, *refs, starts, parts, tile):
    pieces, (out_ref, g) = refs[:-2], refs[-2:]
    fill_mine(g, starts, pieces, parts, tile, 0)
    out_ref[...] = face_ref[0]
    sub = lax.axis_index("sub")
    order = ordered(ids_ref, sub)
    for p in range(PAIR):
        for q in range(PAIR):
            at = pl.multiple_of(order[q] * tile, tile)
            out_ref[order[p], :, pl.ds(at, tile)] -= g[p, :, q * tile : (q + 1) * tile]
    subtract_halo(ids_ref, out_ref, halo_ref, far_of(sub), 0)


def rest_kernel(ids_ref, base_ref, *refs, starts, parts, tile):
    pieces, (out_ref, g) = refs[:-2], refs[-2:]
    count = base_ref.shape[0]
    fill_mine(g, starts, pieces, parts, tile, 0)
    out_ref[...] = base_ref[...]
    order = ordered(ids_ref, lax.axis_index("sub"))
    for p in range(count):
        for q in range(count):
            if p >= PAIR or q >= PAIR:
                at = pl.multiple_of(order[q] * tile, tile)
                out_ref[order[p], :, pl.ds(at, tile)] -= g[p, :, q * tile : (q + 1) * tile]


def finish_kernel(ids_ref, base_ref, halo_ref, out_ref, *, low_tile):
    out_ref[...] = base_ref[...]
    subtract_halo(ids_ref, out_ref, halo_ref, near_of(lax.axis_index("sub")), low_tile)


def assemble(kernel, ids, arrays, shape, scratch):
    smem = pl.BlockSpec(memory_space=pltpu.SMEM)
    vmem = pl.BlockSpec(memory_space=pltpu.VMEM)
    return pl.pallas_call(
        kernel,
        in_specs=[smem] + [vmem] * len(arrays),
        out_shape=jax.ShapeDtypeStruct(shape, F32),
        scratch_shapes=[pltpu.VMEM(scratch, F32)] if scratch else [],
        compiler_params=pltpu.CompilerParams(vmem_limit_bytes=VMEM_LIMIT),
    )(ids, *arrays)


def sizes(count, tile):
    short = tile * LAST[0] // LAST[1]
    return (tile,) * (count - 1) + (tile - short, short)


def shards(factor_blocks, block_inverses, band_offsets, coupling, interface_block, tile_ids):
    rows = lax.axis_size("row")
    subs = lax.axis_size("sub")
    _, count, share, cols = interface_block.shape
    tile = cols // count
    chunks = sizes(count, tile)
    starts = [sum(chunks[:c]) for c in range(len(chunks))]
    offsets = jnp.transpose(band_offsets, (2, 0, 1))
    ids = jnp.transpose(tile_ids)
    far = [(s, s - 1 + 2 * (s % 2)) for s in range(subs)]
    near = [(s, s + 1 - 2 * (s % 2)) for s in range(subs)]
    far, near = ([(s, t) for s, t in pairs if 0 <= t < subs] for pairs in (far, near))
    early = early_solve(ids, block_inverses, coupling) if rows == 2 else None
    ys = list(solve(offsets, ids, factor_blocks, block_inverses, coupling, chunks, tile))
    gain = response(offsets, factor_blocks, block_inverses)
    xs = [early] + ys[1:] if rows == 2 else ys
    first = None
    for stage in range(1, rows):
        recv = []
        for x in xs:
            recv.append(lax.ppermute(x, "row", [(stage - 1, stage)]))
        first = first or recv
        if rows > 2:
            xs = list(update(recv, ys, xs, gain, chunks, stage))
    mine, gain_now = (ys, gain) if rows == 2 else (xs, ())
    kept, own, got = [], [], []
    for c, start in enumerate(starts):
        narrow = share if rows == 2 and start % tile >= share else 0
        piece, kept = gram(
            (first[0], first[1 + c]), (mine[0], mine[1 + c]), gain_now, kept, start, cols, tile, narrow, rows > 2
        )
        if rows == 2:
            got.append(lax.ppermute(kept[0] if narrow else piece, "row", [(1, 0)]))
            own.append(piece)
        else:
            got.append(lax.psum(piece, "row"))
    shape = (count, share, cols)
    last = count - PAIR

    def pick(low, high):
        return got[low:high] + own[low:high]

    message = pair(pick(0, PAIR), starts[:PAIR], rows, tile, share, 0)
    from_far = lax.ppermute(message, "sub", far)
    kernel = functools.partial(middle_kernel, starts=starts[:PAIR], parts=rows, tile=tile)
    base = assemble(kernel, ids, [interface_block, from_far] + pick(0, PAIR), shape, (PAIR, share, PAIR * tile))
    message = pair(pick(last, None), starts[last:], rows, tile, share, last)
    from_near = lax.ppermute(message, "sub", near)
    kernel = functools.partial(rest_kernel, starts=starts[PAIR:], parts=rows, tile=tile)
    base = assemble(kernel, ids, [base] + pick(PAIR, None), shape, shape)
    kernel = functools.partial(finish_kernel, low_tile=last)
    return assemble(kernel, ids, [base, from_near], shape, None)[None]


def solution(mesh):
    return jax.shard_map(
        shards,
        mesh=mesh,
        in_specs=(
            P("sub", "row", None, None, None),
            P("sub", "row", None, None),
            P("sub", "row", None),
            P("sub", "row", None),
            P("sub", None, "row", None),
            P(),
        ),
        out_specs=P("sub", None, "row", None),
        check_vma=False,
    )
```

```python
import functools

import jax
import jax.numpy as jnp
from jax import lax
from jax.experimental import pallas as pl
from jax.experimental.pallas import tpu as pltpu
from jax.sharding import PartitionSpec as P


F32 = jnp.float32
BF16 = jnp.bfloat16
VMEM_LIMIT = 24 * 1024 * 1024
OTHERS = 52 * 1024 * 1024
ALONE = 63 * 1024 * 1024
PAIR = 2
LAST = (3, 8)


def split(x):
    high = x.astype(BF16)
    return high, (x - high.astype(F32)).astype(BF16)


def nt(a, b):
    return lax.dot_general(a, b, (((1,), (1,)), ((), ())), preferred_element_type=F32)


def nn(a, b):
    return lax.dot_general(a, b, (((1,), (0,)), ((), ())), preferred_element_type=F32)


def three(dot, both, high, low):
    rows = both.shape[0] // 2
    wide = dot(both, high)
    return wide[:rows] + (wide[rows:] + dot(both[:rows], low))


def stacked(x):
    return jnp.concatenate(split(x), axis=0)


def near_of(sub):
    return sub + 1 - 2 * (sub % 2)


def far_of(sub):
    return sub - 1 + 2 * (sub % 2)


def shares(ids, k, sub, other):
    count, total = ids.shape
    inside = jnp.logical_and(other >= 0, other < total)
    other = jnp.clip(other, 0, total - 1)
    hit = ids[k, sub] == ids[0, other]
    for i in range(1, count):
        hit = jnp.logical_or(hit, ids[k, sub] == ids[i, other])
    return jnp.logical_and(hit, inside)


def ordered(ids, sub):
    count = ids.shape[0]
    keys = []
    for k in range(count):
        far = shares(ids, k, sub, far_of(sub)).astype(jnp.int32)
        near = shares(ids, k, sub, near_of(sub)).astype(jnp.int32)
        keys.append((1 + near - far) * count + k)
    order = [jnp.int32(0)] * count
    for k in range(count):
        place = sum((keys[j] < keys[k]).astype(jnp.int32) for j in range(count) if j != k)
        order = [jnp.where(place == p, jnp.int32(k), order[p]) for p in range(count)]
    return order


def wait_all(copies):
    for copy in copies:
        copy.wait()


def substitute(off_ref, f, inverse, begin, finish):
    brows, kband = f.shape[0], f.shape[1]
    solved = []
    for i in range(brows):
        rest = begin(i)
        for j in range(i):
            at, found = jnp.int32(0), jnp.bool_(False)
            for band in range(kband):
                same = off_ref[band, 0, i] == i - j
                at = jnp.where(same, jnp.int32(band), at)
                found = jnp.logical_or(found, same)
            block = jnp.where(found, f[i, at], 0.0)
            rest = rest - three(nt, solved[j], *split(block))
        x = three(nt, stacked(rest), *split(inverse[i]))
        solved.append(stacked(x))
        finish(i, x)


def early_kernel(ids_hbm, inv_hbm, b_hbm, out, ids_ref, inverse, b, x_ref, sems):
    @pl.when(lax.axis_index("row") == 0)
    def _():
        size = inverse.shape[0]
        copies = [
            pltpu.make_async_copy(inv_hbm.at[0, 0], inverse, sems.at[0]),
            pltpu.make_async_copy(b_hbm.at[0, pl.ds(0, size)], b, sems.at[1]),
            pltpu.make_async_copy(ids_hbm, ids_ref, sems.at[2]),
        ]
        for copy in copies:
            copy.start()
        copies[1].wait()
        right = stacked(b[...].T)
        copies[0].wait()
        x_ref[...] = three(nt, right, *split(inverse[...]))
        copies[2].wait()
        order = ordered(ids_ref, lax.axis_index("sub"))
        tile = x_ref.shape[0] // len(order)
        writes = []
        for p, k in enumerate(order):
            rows = pl.ds(pl.multiple_of(k * tile, tile), tile)
            writes.append(pltpu.make_async_copy(x_ref.at[rows], out.at[pl.ds(p * tile, tile)], sems.at[3 + p]))
            writes[-1].start()
        wait_all(writes)


def early_solve(ids, inverses, coupling):
    size, cols = inverses.shape[2], coupling.shape[2]
    hbm = pl.BlockSpec(memory_space=pltpu.HBM)
    return pl.pallas_call(
        early_kernel,
        in_specs=[hbm] * 3,
        out_specs=hbm,
        out_shape=jax.ShapeDtypeStruct((cols, size), F32),
        scratch_shapes=[
            pltpu.SMEM(ids.shape, jnp.int32),
            pltpu.VMEM((size, size), F32),
            pltpu.VMEM((size, cols), F32),
            pltpu.VMEM((cols, size), F32),
            pltpu.SemaphoreType.DMA((3 + ids.shape[0],)),
        ],
        compiler_params=pltpu.CompilerParams(vmem_limit_bytes=ALONE),
        cost_estimate=pl.CostEstimate(flops=6 * size * size * cols, bytes_accessed=1 << 20, transcendentals=0),
        name="early",
    )(ids, inverses, coupling)


def solve_kernel(off_ref, ids_ref, f_hbm, inv_hbm, b_hbm, top, *rest, chunks, tiles):
    outs, (f, inverse, b, sems) = rest[: len(chunks)], rest[len(chunks) :]
    brows, _, size, _ = f.shape
    tile = b.shape[2] // tiles

    order = ordered(ids_ref, lax.axis_index("sub"))
    copies = []
    for i in range(brows):
        group = [pltpu.make_async_copy(inv_hbm.at[0, i], inverse.at[i], sems.at[0, i])]
        for p in range(tiles):
            columns = pl.ds(pl.multiple_of(order[p] * tile, tile), tile)
            group.append(
                pltpu.make_async_copy(
                    b_hbm.at[0, pl.ds(i * size, size), columns],
                    b.at[i, :, pl.ds(p * tile, tile)],
                    sems.at[2 + p, i],
                )
            )
        if i > 0:
            group.append(pltpu.make_async_copy(f_hbm.at[0, i], f.at[i], sems.at[1, i]))
        for copy in group:
            copy.start()
        copies.append(group)

    def begin(i):
        wait_all(copies[i])
        return b[i].T

    def finish(i, x):
        if i == 0:
            top[...] = x
            return
        start = 0
        for out, n in zip(outs, chunks):
            out[:, (i - 1) * size : i * size] = x[start : start + n]
            start += n

    substitute(off_ref, f, inverse, begin, finish)


def solve(offsets, ids, blocks, inverses, coupling, chunks, tile):
    _, brows, kband, size, _ = blocks.shape
    total = sum(chunks)
    tiles = total // tile
    hbm = pl.BlockSpec(memory_space=pltpu.HBM)
    smem = pl.BlockSpec(memory_space=pltpu.SMEM)
    return pl.pallas_call(
        functools.partial(solve_kernel, chunks=chunks, tiles=tiles),
        in_specs=[smem, smem, hbm, hbm, hbm],
        out_shape=[jax.ShapeDtypeStruct((total, size), F32)]
        + [jax.ShapeDtypeStruct((n, (brows - 1) * size), F32) for n in chunks],
        scratch_shapes=[
            pltpu.VMEM((brows, kband, size, size), F32),
            pltpu.VMEM((brows, size, size), F32),
            pltpu.VMEM((brows, size, total), F32),
            pltpu.SemaphoreType.DMA((2 + tiles, brows)),
        ],
        compiler_params=pltpu.CompilerParams(vmem_limit_bytes=OTHERS),
        cost_estimate=pl.CostEstimate(flops=6 * 10 * size * size * total, bytes_accessed=8 << 20, transcendentals=0),
        name="others",
    )(offsets, ids, blocks, inverses, coupling)


def response_kernel(off_ref, f_hbm, inv_hbm, gh_ref, gl_ref, f, inverse, acc, sems):
    brows, kband, size, _ = f.shape

    @pl.when(lax.axis_index("row") > 0)
    def _():
        copies = []
        for i in range(brows):
            group = [
                pltpu.make_async_copy(inv_hbm.at[0, i], inverse.at[i], sems.at[0, i]),
                pltpu.make_async_copy(f_hbm.at[0, i], f.at[i], sems.at[1, i]),
            ]
            for copy in group:
                copy.start()
            copies.append(group)

        def begin(i):
            wait_all(copies[i])
            acc[...] = jnp.zeros_like(acc)
            for band in range(kband):
                source = i - off_ref[band, 0, i]

                @pl.when(source < 0)
                def _():
                    at = pl.multiple_of((source + brows) * size, size)
                    acc[pl.ds(at, size), :] += f[i, band].T

            return acc[...]

        def finish(i, x):
            at = slice(i * size, (i + 1) * size)
            gh_ref[:, at], gl_ref[:, at] = split(x)

        substitute(off_ref, f, inverse, begin, finish)


def response(offsets, blocks, inverses):
    _, brows, kband, size, _ = blocks.shape
    width = brows * size
    hbm = pl.BlockSpec(memory_space=pltpu.HBM)
    return pl.pallas_call(
        response_kernel,
        in_specs=[pl.BlockSpec(memory_space=pltpu.SMEM), hbm, hbm],
        out_shape=[jax.ShapeDtypeStruct((width, width), BF16)] * 2,
        scratch_shapes=[
            pltpu.VMEM((brows, kband, size, size), F32),
            pltpu.VMEM((brows, size, size), F32),
            pltpu.VMEM((width, size), F32),
            pltpu.SemaphoreType.DMA((2, brows)),
        ],
        compiler_params=pltpu.CompilerParams(vmem_limit_bytes=VMEM_LIMIT),
        cost_estimate=pl.CostEstimate(flops=6 * 10 * size * size * width, bytes_accessed=8 << 20, transcendentals=0),
        name="response",
    )(offsets, blocks, inverses)


def update_kernel(*refs, chunks, stage):
    gh_ref, gl_ref = refs[:2]
    width = 1 + len(chunks)
    recv, y, cur, out = (refs[2 + k * width : 2 + (k + 1) * width] for k in range(4))
    for source, target in zip(cur, out):
        target[...] = source[...]

    @pl.when(lax.axis_index("row") == stage)
    def _():
        size = recv[0].shape[1]
        start = 0
        for c, n in enumerate(chunks):
            rows = slice(start, start + n)
            given = jnp.concatenate([recv[0][rows], recv[1 + c][...]], axis=1)
            change = three(nn, stacked(given), gh_ref[...], gl_ref[...])
            out[0][rows] = y[0][rows] - change[:, :size]
            out[1 + c][...] = y[1 + c][...] - change[:, size:]
            start += n


def update(recv, y, cur, gain, chunks, stage):
    return pl.pallas_call(
        functools.partial(update_kernel, chunks=chunks, stage=stage),
        out_shape=[jax.ShapeDtypeStruct(x.shape, F32) for x in y],
        compiler_params=pltpu.CompilerParams(vmem_limit_bytes=VMEM_LIMIT),
        name="update",
    )(*gain, *recv, *y, *cur)


def gram_kernel(*refs, start, fused, clear, last, share, tile):
    recv0_ref, recv_ref, y0_ref, y_ref = refs[:4]
    refs = refs[4:]
    if fused:
        gh_ref, gl_ref = refs[:2]
        refs = refs[2:]
    if start:
        oldh_ref, oldl_ref = refs[:2]
        refs = refs[2:]
    piece, rest = refs[0], refs[1:]
    n = recv_ref.shape[0]
    here = slice(start, start + n)

    @pl.when(lax.axis_index("row") > 0)
    def _():
        recv = stacked(jnp.concatenate([recv0_ref[here], recv_ref[...]], axis=1))
        x = jnp.concatenate([y0_ref[here], y_ref[...]], axis=1)
        if fused:
            x = x - three(nn, recv, gh_ref[...], gl_ref[...])
        x = stacked(x)
        high = jnp.concatenate([recv[:n], x[:n]], axis=1)
        low = jnp.concatenate([recv[n:], x[n:]], axis=1)
        both = jnp.concatenate([high, low], axis=0)
        if start:
            piece[:, :start] = three(nn, both, oldh_ref[:, :start], oldl_ref[:, :start])
        piece[:, here] = three(nt, both, high, low)
        if not last:
            rest[0][:, here] = high.T
            rest[1][:, here] = low.T
        elif share:
            rest[0][...] = jnp.concatenate(
                [piece[:, t * tile : t * tile + share] for t in range((start + n) // tile)], axis=1
            )

    if clear:

        @pl.when(lax.axis_index("row") == 0)
        def _():
            piece[...] = jnp.zeros_like(piece)


def gram(recv, y, gain, kept, start, total, tile, share, clear):
    n = recv[1].shape[0]
    half = recv[0].shape[1] + recv[1].shape[1]
    last = start + n == total
    inputs = [*recv, *y, *gain, *kept]
    if not last:
        more = [jax.ShapeDtypeStruct((2 * half, total), BF16)] * 2
    else:
        more = [jax.ShapeDtypeStruct((n, total // tile * share), F32)] if share else []
    results = pl.pallas_call(
        functools.partial(
            gram_kernel, start=start, fused=bool(gain), clear=clear, last=last, share=share, tile=tile
        ),
        in_specs=[pl.BlockSpec(memory_space=pltpu.VMEM)] * len(inputs),
        out_shape=[jax.ShapeDtypeStruct((n, start + n), F32)] + more,
        input_output_aliases={len(inputs) - 2 + i: 1 + i for i in range(2)} if start and not last else {},
        compiler_params=pltpu.CompilerParams(vmem_limit_bytes=VMEM_LIMIT),
        cost_estimate=pl.CostEstimate(
            flops=6 * n * half * (half + 2 * (start + n)), bytes_accessed=4 << 20, transcendentals=0
        ),
    )(*inputs)
    return results[0], list(results[1:])


def fill(out, chunks, part, tile, low_tile):
    share = out.shape[1]
    low, high = part * share, (part + 1) * share
    base = low_tile * tile
    for start, piece in chunks:
        n = piece.shape[0]
        at, inner = start // tile, start % tile
        if piece.shape[1] < start + n:
            turned = piece[:, low_tile * share :].T
            for t in range(low_tile, at + 1):
                first = (t - low_tile) * share
                out[t - low_tile, :, start - base : start - base + n] = turned[first : first + share]
            continue
        first, stop = max(inner, low), min(inner + n, high)
        if first < stop:
            out[at - low_tile, first - low : stop - low, : start + n - base] = piece[first - inner : stop - inner, base:]
        if start > base:
            turned = piece[:, base:start].T
            for t in range(low_tile, -(-start // tile)):
                first, stop = t * tile + low, min(t * tile + high, start)
                if first < stop:
                    out[t - low_tile, : stop - first, start - base : start - base + n] = turned[
                        first - base : stop - base
                    ]


def fill_mine(out, starts, pieces, parts, tile, low_tile):
    row = lax.axis_index("row")
    both = len(pieces) > len(starts)
    for part in range(parts):
        mine = pieces[len(starts) :] if both and part else pieces[: len(starts)]
        pl.when(row == part)(functools.partial(fill, out, list(zip(starts, mine)), part, tile, low_tile))


def pair_kernel(*refs, starts, parts, tile, low_tile):
    fill_mine(refs[-1], starts, refs[:-1], parts, tile, low_tile)


def pair(pieces, starts, parts, tile, share, low_tile):
    return pl.pallas_call(
        functools.partial(pair_kernel, starts=starts, parts=parts, tile=tile, low_tile=low_tile),
        out_shape=jax.ShapeDtypeStruct((PAIR, share, PAIR * tile), F32),
        compiler_params=pltpu.CompilerParams(vmem_limit_bytes=VMEM_LIMIT),
    )(*pieces)


def subtract_halo(ids, out, halo, other, low_tile):
    count, total = ids.shape
    tile = halo.shape[2] // PAIR
    sub = lax.axis_index("sub")
    inside = jnp.logical_and(other >= 0, other < total)
    other = jnp.clip(other, 0, total - 1)
    order = ordered(ids, other)
    slots = []
    for m in range(PAIR):
        number = ids[order[low_tile + m], other]
        place, hit = jnp.int32(0), jnp.bool_(False)
        for i in range(count):
            same = ids[i, sub] == number
            place = jnp.where(same, jnp.int32(i), place)
            hit = jnp.logical_or(hit, same)
        slots.append((place, jnp.logical_and(hit, inside)))
    for m in range(PAIR):
        for n in range(PAIR):

            @pl.when(jnp.logical_and(slots[m][1], slots[n][1]))
            def _():
                at = pl.multiple_of(slots[n][0] * tile, tile)
                out[slots[m][0], :, pl.ds(at, tile)] -= halo[m, :, n * tile : (n + 1) * tile]


def subtract_gram(ids_ref, out, g, chunks, parts, tile, blocks):
    starts, pieces = chunks
    for p, q in blocks:
        g[p, :, q * tile : (q + 1) * tile] = jnp.zeros((g.shape[1], tile), F32)
    fill_mine(g, starts, pieces, parts, tile, 0)
    order = ordered(ids_ref, lax.axis_index("sub"))
    for p, q in blocks:
        at = pl.multiple_of(order[q] * tile, tile)
        out[order[p], :, pl.ds(at, tile)] -= g[p, :, q * tile : (q + 1) * tile]


def middle_kernel(ids_ref, face_ref, halo_ref, *refs, starts, parts, tile):
    pieces, (out_ref, g) = refs[:-2], refs[-2:]
    count = out_ref.shape[0]
    out_ref[...] = face_ref[0]
    blocks = [(p, q) for p in range(count) for q in range(count)]
    subtract_gram(ids_ref, out_ref, g, (starts, pieces), parts, tile, blocks)
    subtract_halo(ids_ref, out_ref, halo_ref, far_of(lax.axis_index("sub")), 0)


def finish_kernel(ids_ref, base_ref, halo_ref, *refs, starts, parts, tile, low_tile):
    pieces, (out_ref, g) = refs[:-2], refs[-2:]
    count = out_ref.shape[0]
    last = count - 1
    out_ref[...] = base_ref[...]
    blocks = [(p, q) for p in range(count) for q in range(count) if last in (p, q)]
    subtract_gram(ids_ref, out_ref, g, (starts, pieces), parts, tile, blocks)
    subtract_halo(ids_ref, out_ref, halo_ref, near_of(lax.axis_index("sub")), low_tile)


def assemble(kernel, ids, arrays, shape, scratch):
    smem = pl.BlockSpec(memory_space=pltpu.SMEM)
    vmem = pl.BlockSpec(memory_space=pltpu.VMEM)
    return pl.pallas_call(
        kernel,
        in_specs=[smem] + [vmem] * len(arrays),
        out_shape=jax.ShapeDtypeStruct(shape, F32),
        scratch_shapes=[pltpu.VMEM(scratch, F32)] if scratch else [],
        compiler_params=pltpu.CompilerParams(vmem_limit_bytes=VMEM_LIMIT),
    )(ids, *arrays)


def sizes(count, tile):
    short = tile * LAST[0] // LAST[1]
    return (tile,) * (count - 1) + (tile - short, short)


def shards(factor_blocks, block_inverses, band_offsets, coupling, interface_block, tile_ids):
    rows = lax.axis_size("row")
    subs = lax.axis_size("sub")
    _, count, share, cols = interface_block.shape
    tile = cols // count
    chunks = sizes(count, tile)
    starts = [sum(chunks[:c]) for c in range(len(chunks))]
    offsets = jnp.transpose(band_offsets, (2, 0, 1))
    ids = jnp.transpose(tile_ids)
    far = [(s, s - 1 + 2 * (s % 2)) for s in range(subs)]
    near = [(s, s + 1 - 2 * (s % 2)) for s in range(subs)]
    far, near = ([(s, t) for s, t in pairs if 0 <= t < subs] for pairs in (far, near))
    early = early_solve(ids, block_inverses, coupling) if rows == 2 else None
    ys = list(solve(offsets, ids, factor_blocks, block_inverses, coupling, chunks, tile))
    gain = response(offsets, factor_blocks, block_inverses)
    xs = [early] + ys[1:] if rows == 2 else ys
    first = None
    for stage in range(1, rows):
        recv = []
        for x in xs:
            recv.append(lax.ppermute(x, "row", [(stage - 1, stage)]))
        first = first or recv
        if rows > 2:
            xs = list(update(recv, ys, xs, gain, chunks, stage))
    mine, gain_now = (ys, gain) if rows == 2 else (xs, ())
    kept, own, got = [], [], []
    for c, start in enumerate(starts):
        narrow = share if rows == 2 and start % tile >= share else 0
        piece, kept = gram(
            (first[0], first[1 + c]), (mine[0], mine[1 + c]), gain_now, kept, start, cols, tile, narrow, rows > 2
        )
        if rows == 2:
            got.append(lax.ppermute(kept[0] if narrow else piece, "row", [(1, 0)]))
            own.append(piece)
        else:
            got.append(lax.psum(piece, "row"))
    shape = (count, share, cols)
    last = count - PAIR

    def pick(low, high):
        return got[low:high] + own[low:high]

    message = pair(pick(0, PAIR), starts[:PAIR], rows, tile, share, 0)
    from_far = lax.ppermute(message, "sub", far)
    kernel = functools.partial(middle_kernel, starts=starts[:-1], parts=rows, tile=tile)
    arrays = [interface_block, from_far] + got[:-1] + own[:-1]
    base = assemble(kernel, ids, arrays, shape, shape)
    message = pair(pick(last, None), starts[last:], rows, tile, share, last)
    from_near = lax.ppermute(message, "sub", near)
    kernel = functools.partial(finish_kernel, starts=starts[-1:], parts=rows, tile=tile, low_tile=last)
    return assemble(kernel, ids, [base, from_near] + pick(-1, None), shape, shape)[None]


def solution(mesh):
    return jax.shard_map(
        shards,
        mesh=mesh,
        in_specs=(
            P("sub", "row", None, None, None),
            P("sub", "row", None, None),
            P("sub", "row", None),
            P("sub", "row", None),
            P("sub", None, "row", None),
            P(),
        ),
        out_specs=P("sub", None, "row", None),
        check_vma=False,
    )
```

```python
import functools

import jax
import jax.numpy as jnp
from jax import lax
from jax.experimental import pallas as pl
from jax.experimental.pallas import tpu as pltpu
from jax.sharding import PartitionSpec as P


F32 = jnp.float32
BF16 = jnp.bfloat16
VMEM_LIMIT = 24 * 1024 * 1024
OTHERS = 52 * 1024 * 1024
ALONE = 63 * 1024 * 1024
PAIR = 2
LAST = (1, 2)


def split(x):
    high = x.astype(BF16)
    return high, (x - high.astype(F32)).astype(BF16)


def nt(a, b):
    return lax.dot_general(a, b, (((1,), (1,)), ((), ())), preferred_element_type=F32)


def nn(a, b):
    return lax.dot_general(a, b, (((1,), (0,)), ((), ())), preferred_element_type=F32)


def three(dot, both, high, low):
    rows = both.shape[0] // 2
    wide = dot(both, high)
    return wide[:rows] + (wide[rows:] + dot(both[:rows], low))


def stacked(x):
    return jnp.concatenate(split(x), axis=0)


def near_of(sub):
    return sub + 1 - 2 * (sub % 2)


def far_of(sub):
    return sub - 1 + 2 * (sub % 2)


def shares(ids, k, sub, other):
    count, total = ids.shape
    inside = jnp.logical_and(other >= 0, other < total)
    other = jnp.clip(other, 0, total - 1)
    hit = ids[k, sub] == ids[0, other]
    for i in range(1, count):
        hit = jnp.logical_or(hit, ids[k, sub] == ids[i, other])
    return jnp.logical_and(hit, inside)


def ordered(ids, sub):
    count = ids.shape[0]
    keys = []
    for k in range(count):
        far = shares(ids, k, sub, far_of(sub)).astype(jnp.int32)
        near = shares(ids, k, sub, near_of(sub)).astype(jnp.int32)
        keys.append((1 + near - far) * count + k)
    order = [jnp.int32(0)] * count
    for k in range(count):
        place = sum((keys[j] < keys[k]).astype(jnp.int32) for j in range(count) if j != k)
        order = [jnp.where(place == p, jnp.int32(k), order[p]) for p in range(count)]
    return order


def wait_all(copies):
    for copy in copies:
        copy.wait()


def substitute(off_ref, f, inverse, begin, finish):
    brows, kband = f.shape[0], f.shape[1]
    solved = []
    for i in range(brows):
        rest = begin(i)
        for j in range(i):
            at, found = jnp.int32(0), jnp.bool_(False)
            for band in range(kband):
                same = off_ref[band, 0, i] == i - j
                at = jnp.where(same, jnp.int32(band), at)
                found = jnp.logical_or(found, same)
            block = jnp.where(found, f[i, at], 0.0)
            rest = rest - three(nt, solved[j], *split(block))
        x = three(nt, stacked(rest), *split(inverse[i]))
        solved.append(stacked(x))
        finish(i, x)


def early_kernel(ids_hbm, inv_hbm, b_hbm, out, ids_ref, inverse, b, x_ref, sems):
    @pl.when(lax.axis_index("row") == 0)
    def _():
        size = inverse.shape[0]
        copies = [
            pltpu.make_async_copy(inv_hbm.at[0, 0], inverse, sems.at[0]),
            pltpu.make_async_copy(b_hbm.at[0, pl.ds(0, size)], b, sems.at[1]),
            pltpu.make_async_copy(ids_hbm, ids_ref, sems.at[2]),
        ]
        for copy in copies:
            copy.start()
        copies[1].wait()
        right = stacked(b[...].T)
        copies[0].wait()
        x_ref[...] = three(nt, right, *split(inverse[...]))
        copies[2].wait()
        order = ordered(ids_ref, lax.axis_index("sub"))
        tile = x_ref.shape[0] // len(order)
        writes = []
        for p, k in enumerate(order):
            rows = pl.ds(pl.multiple_of(k * tile, tile), tile)
            writes.append(pltpu.make_async_copy(x_ref.at[rows], out.at[pl.ds(p * tile, tile)], sems.at[3 + p]))
            writes[-1].start()
        wait_all(writes)


def early_solve(ids, inverses, coupling):
    size, cols = inverses.shape[2], coupling.shape[2]
    hbm = pl.BlockSpec(memory_space=pltpu.HBM)
    return pl.pallas_call(
        early_kernel,
        in_specs=[hbm] * 3,
        out_specs=hbm,
        out_shape=jax.ShapeDtypeStruct((cols, size), F32),
        scratch_shapes=[
            pltpu.SMEM(ids.shape, jnp.int32),
            pltpu.VMEM((size, size), F32),
            pltpu.VMEM((size, cols), F32),
            pltpu.VMEM((cols, size), F32),
            pltpu.SemaphoreType.DMA((3 + ids.shape[0],)),
        ],
        compiler_params=pltpu.CompilerParams(vmem_limit_bytes=ALONE),
        cost_estimate=pl.CostEstimate(flops=6 * size * size * cols, bytes_accessed=1 << 20, transcendentals=0),
        name="early",
    )(ids, inverses, coupling)


def solve_kernel(off_ref, ids_ref, f_hbm, inv_hbm, b_hbm, top, *rest, chunks, tiles):
    outs, (f, inverse, b, sems) = rest[: len(chunks)], rest[len(chunks) :]
    brows, _, size, _ = f.shape
    tile = b.shape[2] // tiles

    order = ordered(ids_ref, lax.axis_index("sub"))
    copies = []
    for i in range(brows):
        group = [pltpu.make_async_copy(inv_hbm.at[0, i], inverse.at[i], sems.at[0, i])]
        for p in range(tiles):
            columns = pl.ds(pl.multiple_of(order[p] * tile, tile), tile)
            group.append(
                pltpu.make_async_copy(
                    b_hbm.at[0, pl.ds(i * size, size), columns],
                    b.at[i, :, pl.ds(p * tile, tile)],
                    sems.at[2 + p, i],
                )
            )
        if i > 0:
            group.append(pltpu.make_async_copy(f_hbm.at[0, i], f.at[i], sems.at[1, i]))
        for copy in group:
            copy.start()
        copies.append(group)

    def begin(i):
        wait_all(copies[i])
        return b[i].T

    def finish(i, x):
        if i == 0:
            top[...] = x
            return
        start = 0
        for out, n in zip(outs, chunks):
            out[:, (i - 1) * size : i * size] = x[start : start + n]
            start += n

    substitute(off_ref, f, inverse, begin, finish)


def solve(offsets, ids, blocks, inverses, coupling, chunks, tile):
    _, brows, kband, size, _ = blocks.shape
    total = sum(chunks)
    tiles = total // tile
    hbm = pl.BlockSpec(memory_space=pltpu.HBM)
    smem = pl.BlockSpec(memory_space=pltpu.SMEM)
    return pl.pallas_call(
        functools.partial(solve_kernel, chunks=chunks, tiles=tiles),
        in_specs=[smem, smem, hbm, hbm, hbm],
        out_shape=[jax.ShapeDtypeStruct((total, size), F32)]
        + [jax.ShapeDtypeStruct((n, (brows - 1) * size), F32) for n in chunks],
        scratch_shapes=[
            pltpu.VMEM((brows, kband, size, size), F32),
            pltpu.VMEM((brows, size, size), F32),
            pltpu.VMEM((brows, size, total), F32),
            pltpu.SemaphoreType.DMA((2 + tiles, brows)),
        ],
        compiler_params=pltpu.CompilerParams(vmem_limit_bytes=OTHERS),
        cost_estimate=pl.CostEstimate(flops=6 * 10 * size * size * total, bytes_accessed=8 << 20, transcendentals=0),
        name="others",
    )(offsets, ids, blocks, inverses, coupling)


def response_kernel(off_ref, f_hbm, inv_hbm, gh_ref, gl_ref, f, inverse, acc, sems):
    brows, kband, size, _ = f.shape

    @pl.when(lax.axis_index("row") > 0)
    def _():
        copies = []
        for i in range(brows):
            group = [
                pltpu.make_async_copy(inv_hbm.at[0, i], inverse.at[i], sems.at[0, i]),
                pltpu.make_async_copy(f_hbm.at[0, i], f.at[i], sems.at[1, i]),
            ]
            for copy in group:
                copy.start()
            copies.append(group)

        def begin(i):
            wait_all(copies[i])
            acc[...] = jnp.zeros_like(acc)
            for band in range(kband):
                source = i - off_ref[band, 0, i]

                @pl.when(source < 0)
                def _():
                    at = pl.multiple_of((source + brows) * size, size)
                    acc[pl.ds(at, size), :] += f[i, band].T

            return acc[...]

        def finish(i, x):
            at = slice(i * size, (i + 1) * size)
            gh_ref[:, at], gl_ref[:, at] = split(x)

        substitute(off_ref, f, inverse, begin, finish)


def response(offsets, blocks, inverses):
    _, brows, kband, size, _ = blocks.shape
    width = brows * size
    hbm = pl.BlockSpec(memory_space=pltpu.HBM)
    return pl.pallas_call(
        response_kernel,
        in_specs=[pl.BlockSpec(memory_space=pltpu.SMEM), hbm, hbm],
        out_shape=[jax.ShapeDtypeStruct((width, width), BF16)] * 2,
        scratch_shapes=[
            pltpu.VMEM((brows, kband, size, size), F32),
            pltpu.VMEM((brows, size, size), F32),
            pltpu.VMEM((width, size), F32),
            pltpu.SemaphoreType.DMA((2, brows)),
        ],
        compiler_params=pltpu.CompilerParams(vmem_limit_bytes=VMEM_LIMIT),
        cost_estimate=pl.CostEstimate(flops=6 * 10 * size * size * width, bytes_accessed=8 << 20, transcendentals=0),
        name="response",
    )(offsets, blocks, inverses)


def update_kernel(*refs, chunks, stage):
    gh_ref, gl_ref = refs[:2]
    width = 1 + len(chunks)
    recv, y, cur, out = (refs[2 + k * width : 2 + (k + 1) * width] for k in range(4))
    for source, target in zip(cur, out):
        target[...] = source[...]

    @pl.when(lax.axis_index("row") == stage)
    def _():
        size = recv[0].shape[1]
        start = 0
        for c, n in enumerate(chunks):
            rows = slice(start, start + n)
            given = jnp.concatenate([recv[0][rows], recv[1 + c][...]], axis=1)
            change = three(nn, stacked(given), gh_ref[...], gl_ref[...])
            out[0][rows] = y[0][rows] - change[:, :size]
            out[1 + c][...] = y[1 + c][...] - change[:, size:]
            start += n


def update(recv, y, cur, gain, chunks, stage):
    return pl.pallas_call(
        functools.partial(update_kernel, chunks=chunks, stage=stage),
        out_shape=[jax.ShapeDtypeStruct(x.shape, F32) for x in y],
        compiler_params=pltpu.CompilerParams(vmem_limit_bytes=VMEM_LIMIT),
        name="update",
    )(*gain, *recv, *y, *cur)


def gram_kernel(*refs, start, fused, clear, last, share, tile):
    recv0_ref, recv_ref, y0_ref, y_ref = refs[:4]
    refs = refs[4:]
    if fused:
        gh_ref, gl_ref = refs[:2]
        refs = refs[2:]
    if start:
        oldh_ref, oldl_ref = refs[:2]
        refs = refs[2:]
    piece, rest = refs[0], refs[1:]
    n = recv_ref.shape[0]
    here = slice(start, start + n)

    @pl.when(lax.axis_index("row") > 0)
    def _():
        recv = stacked(jnp.concatenate([recv0_ref[here], recv_ref[...]], axis=1))
        x = jnp.concatenate([y0_ref[here], y_ref[...]], axis=1)
        if fused:
            x = x - three(nn, recv, gh_ref[...], gl_ref[...])
        x = stacked(x)
        high = jnp.concatenate([recv[:n], x[:n]], axis=1)
        low = jnp.concatenate([recv[n:], x[n:]], axis=1)
        both = jnp.concatenate([high, low], axis=0)
        if start:
            piece[:, :start] = three(nn, both, oldh_ref[:, :start], oldl_ref[:, :start])
        piece[:, here] = three(nt, both, high, low)
        if not last:
            rest[0][:, here] = high.T
            rest[1][:, here] = low.T
        elif share:
            rest[0][...] = jnp.concatenate(
                [piece[:, t * tile : t * tile + share] for t in range((start + n) // tile)], axis=1
            )

    if clear:

        @pl.when(lax.axis_index("row") == 0)
        def _():
            piece[...] = jnp.zeros_like(piece)


def gram(recv, y, gain, kept, start, total, tile, share, clear):
    n = recv[1].shape[0]
    half = recv[0].shape[1] + recv[1].shape[1]
    last = start + n == total
    inputs = [*recv, *y, *gain, *kept]
    if not last:
        more = [jax.ShapeDtypeStruct((2 * half, total), BF16)] * 2
    else:
        more = [jax.ShapeDtypeStruct((n, total // tile * share), F32)] if share else []
    results = pl.pallas_call(
        functools.partial(
            gram_kernel, start=start, fused=bool(gain), clear=clear, last=last, share=share, tile=tile
        ),
        in_specs=[pl.BlockSpec(memory_space=pltpu.VMEM)] * len(inputs),
        out_shape=[jax.ShapeDtypeStruct((n, start + n), F32)] + more,
        input_output_aliases={len(inputs) - 2 + i: 1 + i for i in range(2)} if start and not last else {},
        compiler_params=pltpu.CompilerParams(vmem_limit_bytes=VMEM_LIMIT),
        cost_estimate=pl.CostEstimate(
            flops=6 * n * half * (half + 2 * (start + n)), bytes_accessed=4 << 20, transcendentals=0
        ),
    )(*inputs)
    return results[0], list(results[1:])


def fill(out, chunks, part, tile, low_tile):
    share = out.shape[1]
    low, high = part * share, (part + 1) * share
    base = low_tile * tile
    for start, piece in chunks:
        n = piece.shape[0]
        at, inner = start // tile, start % tile
        if piece.shape[1] < start + n:
            turned = piece[:, low_tile * share :].T
            for t in range(low_tile, at + 1):
                first = (t - low_tile) * share
                out[t - low_tile, :, start - base : start - base + n] = turned[first : first + share]
            continue
        first, stop = max(inner, low), min(inner + n, high)
        if first < stop:
            out[at - low_tile, first - low : stop - low, : start + n - base] = piece[first - inner : stop - inner, base:]
        if start > base:
            turned = piece[:, base:start].T
            for t in range(low_tile, -(-start // tile)):
                first, stop = t * tile + low, min(t * tile + high, start)
                if first < stop:
                    out[t - low_tile, : stop - first, start - base : start - base + n] = turned[
                        first - base : stop - base
                    ]


def fill_mine(out, starts, pieces, parts, tile, low_tile):
    row = lax.axis_index("row")
    both = len(pieces) > len(starts)
    for part in range(parts):
        mine = pieces[len(starts) :] if both and part else pieces[: len(starts)]
        pl.when(row == part)(functools.partial(fill, out, list(zip(starts, mine)), part, tile, low_tile))


def pair_kernel(*refs, starts, parts, tile, low_tile):
    fill_mine(refs[-1], starts, refs[:-1], parts, tile, low_tile)


def pair(pieces, starts, parts, tile, share, low_tile):
    return pl.pallas_call(
        functools.partial(pair_kernel, starts=starts, parts=parts, tile=tile, low_tile=low_tile),
        out_shape=jax.ShapeDtypeStruct((PAIR, share, PAIR * tile), F32),
        compiler_params=pltpu.CompilerParams(vmem_limit_bytes=VMEM_LIMIT),
    )(*pieces)


def matches(ids, other, low_tile):
    count, total = ids.shape
    sub = lax.axis_index("sub")
    inside = jnp.logical_and(other >= 0, other < total)
    other = jnp.clip(other, 0, total - 1)
    order = ordered(ids, other)
    slots = []
    for m in range(PAIR):
        number = ids[order[low_tile + m], other]
        place, hit = jnp.int32(0), jnp.bool_(False)
        for i in range(count):
            same = ids[i, sub] == number
            place = jnp.where(same, jnp.int32(i), place)
            hit = jnp.logical_or(hit, same)
        slots.append((place, jnp.logical_and(hit, inside)))
    return slots


def subtract_halo(ids, out, halo, other, low_tile):
    tile = halo.shape[2] // PAIR
    slots = matches(ids, other, low_tile)
    for m in range(PAIR):
        for n in range(PAIR):

            @pl.when(jnp.logical_and(slots[m][1], slots[n][1]))
            def _():
                at = pl.multiple_of(slots[n][0] * tile, tile)
                out[slots[m][0], :, pl.ds(at, tile)] -= halo[m, :, n * tile : (n + 1) * tile]


def subtract_gram(ids_ref, out, g, chunks, parts, tile, blocks):
    starts, pieces = chunks
    for p, q in blocks:
        g[p, :, q * tile : (q + 1) * tile] = jnp.zeros((g.shape[1], tile), F32)
    fill_mine(g, starts, pieces, parts, tile, 0)
    order = ordered(ids_ref, lax.axis_index("sub"))
    for p, q in blocks:
        at = pl.multiple_of(order[q] * tile, tile)
        out[order[p], :, pl.ds(at, tile)] -= g[p, :, q * tile : (q + 1) * tile]


def middle_kernel(ids_ref, face_ref, halo_ref, *refs, starts, parts, tile):
    pieces, (out_ref, g) = refs[:-2], refs[-2:]
    count = out_ref.shape[0]
    out_ref[...] = face_ref[0]
    blocks = [(p, q) for p in range(count) for q in range(count)]
    subtract_gram(ids_ref, out_ref, g, (starts, pieces), parts, tile, blocks)
    subtract_halo(ids_ref, out_ref, halo_ref, far_of(lax.axis_index("sub")), 0)


def rest_kernel(ids_ref, base_ref, *refs, starts, parts, tile, low_tile):
    pieces, (out_ref, weight_ref, g) = refs[:-3], refs[-3:]
    count = out_ref.shape[0]
    last = count - 1
    out_ref[...] = base_ref[...]
    blocks = [(p, q) for p in range(count) for q in range(count) if last in (p, q)]
    subtract_gram(ids_ref, out_ref, g, (starts, pieces), parts, tile, blocks)
    slots = matches(ids_ref, near_of(lax.axis_index("sub")), low_tile)
    for m, (place, hit) in enumerate(slots):
        for i in range(count):
            weight = jnp.logical_and(hit, place == i).astype(F32)
            weight_ref[m, i] = jnp.full(weight_ref.shape[2:], weight, F32)


def finish_kernel(base_ref, halo_ref, weight_ref, out_ref):
    count, _, cols = base_ref.shape
    tile = cols // count
    for i in range(count):
        left = [weight_ref[m, i, 0:1] for m in range(PAIR)]
        for j in range(count):
            right = [weight_ref[n, j, 0:1] for n in range(PAIR)]
            block = base_ref[i, :, j * tile : (j + 1) * tile]
            for m in range(PAIR):
                for n in range(PAIR):
                    block = block - (left[m] * right[n]) * halo_ref[m, :, n * tile : (n + 1) * tile]
            out_ref[i, :, j * tile : (j + 1) * tile] = block


def assemble(kernel, ids, arrays, shapes, scratch):
    smem = pl.BlockSpec(memory_space=pltpu.SMEM)
    vmem = pl.BlockSpec(memory_space=pltpu.VMEM)
    return pl.pallas_call(
        kernel,
        in_specs=[smem] * len(ids) + [vmem] * len(arrays),
        out_shape=[jax.ShapeDtypeStruct(shape, F32) for shape in shapes],
        scratch_shapes=[pltpu.VMEM(scratch, F32)] if scratch else [],
        compiler_params=pltpu.CompilerParams(vmem_limit_bytes=VMEM_LIMIT),
    )(*ids, *arrays)


def sizes(count, tile):
    short = tile * LAST[0] // LAST[1]
    return (tile,) * (count - 1) + (tile - short, short)


def shards(factor_blocks, block_inverses, band_offsets, coupling, interface_block, tile_ids):
    rows = lax.axis_size("row")
    subs = lax.axis_size("sub")
    _, count, share, cols = interface_block.shape
    tile = cols // count
    chunks = sizes(count, tile)
    starts = [sum(chunks[:c]) for c in range(len(chunks))]
    offsets = jnp.transpose(band_offsets, (2, 0, 1))
    ids = jnp.transpose(tile_ids)
    far = [(s, s - 1 + 2 * (s % 2)) for s in range(subs)]
    near = [(s, s + 1 - 2 * (s % 2)) for s in range(subs)]
    far, near = ([(s, t) for s, t in pairs if 0 <= t < subs] for pairs in (far, near))
    early = early_solve(ids, block_inverses, coupling) if rows == 2 else None
    ys = list(solve(offsets, ids, factor_blocks, block_inverses, coupling, chunks, tile))
    gain = response(offsets, factor_blocks, block_inverses)
    xs = [early] + ys[1:] if rows == 2 else ys
    first = None
    for stage in range(1, rows):
        recv = []
        for x in xs:
            recv.append(lax.ppermute(x, "row", [(stage - 1, stage)]))
        first = first or recv
        if rows > 2:
            xs = list(update(recv, ys, xs, gain, chunks, stage))
    mine, gain_now = (ys, gain) if rows == 2 else (xs, ())
    kept, own, got = [], [], []
    for c, start in enumerate(starts):
        narrow = share if rows == 2 and start % tile >= share else 0
        piece, kept = gram(
            (first[0], first[1 + c]), (mine[0], mine[1 + c]), gain_now, kept, start, cols, tile, narrow, rows > 2
        )
        if rows == 2:
            got.append(lax.ppermute(kept[0] if narrow else piece, "row", [(1, 0)]))
            own.append(piece)
        else:
            got.append(lax.psum(piece, "row"))
    shape = (count, share, cols)
    last = count - PAIR

    def pick(low, high):
        return got[low:high] + own[low:high]

    message = pair(pick(0, PAIR), starts[:PAIR], rows, tile, share, 0)
    from_far = lax.ppermute(message, "sub", far)
    kernel = functools.partial(middle_kernel, starts=starts[:-1], parts=rows, tile=tile)
    arrays = [interface_block, from_far] + got[:-1] + own[:-1]
    (base,) = assemble(kernel, [ids], arrays, [shape], shape)
    message = pair(pick(last, None), starts[last:], rows, tile, share, last)
    from_near = lax.ppermute(message, "sub", near)
    kernel = functools.partial(rest_kernel, starts=starts[-1:], parts=rows, tile=tile, low_tile=last)
    arrays = [base] + pick(-1, None)
    base, weights = assemble(kernel, [ids], arrays, [shape, (PAIR, count, 8, tile)], shape)
    (out,) = assemble(finish_kernel, [], [base, from_near, weights], [shape], None)
    return out[None]


def solution(mesh):
    return jax.shard_map(
        shards,
        mesh=mesh,
        in_specs=(
            P("sub", "row", None, None, None),
            P("sub", "row", None, None),
            P("sub", "row", None),
            P("sub", "row", None),
            P("sub", None, "row", None),
            P(),
        ),
        out_specs=P("sub", None, "row", None),
        check_vma=False,
    )
```

```python
import functools

import jax
import jax.numpy as jnp
from jax import lax
from jax.experimental import pallas as pl
from jax.experimental.pallas import tpu as pltpu
from jax.sharding import PartitionSpec as P


F32 = jnp.float32
BF16 = jnp.bfloat16
VMEM_LIMIT = 24 * 1024 * 1024
OTHERS = 52 * 1024 * 1024
ALONE = 53 * 1024 * 1024
PAIR = 2
LAST = (1, 2)


def split(x):
    high = x.astype(BF16)
    return high, (x - high.astype(F32)).astype(BF16)


def nt(a, b):
    return lax.dot_general(a, b, (((1,), (1,)), ((), ())), preferred_element_type=F32)


def nn(a, b):
    return lax.dot_general(a, b, (((1,), (0,)), ((), ())), preferred_element_type=F32)


def three(dot, both, high, low):
    rows = both.shape[0] // 2
    wide = dot(both, high)
    return wide[:rows] + (wide[rows:] + dot(both[:rows], low))


def stacked(x):
    return jnp.concatenate(split(x), axis=0)


def near_of(sub):
    return sub + 1 - 2 * (sub % 2)


def far_of(sub):
    return sub - 1 + 2 * (sub % 2)


def shares(ids, k, sub, other):
    count, total = ids.shape
    inside = jnp.logical_and(other >= 0, other < total)
    other = jnp.clip(other, 0, total - 1)
    hit = ids[k, sub] == ids[0, other]
    for i in range(1, count):
        hit = jnp.logical_or(hit, ids[k, sub] == ids[i, other])
    return jnp.logical_and(hit, inside)


def ordered(ids, sub):
    count = ids.shape[0]
    keys = []
    for k in range(count):
        far = shares(ids, k, sub, far_of(sub)).astype(jnp.int32)
        near = shares(ids, k, sub, near_of(sub)).astype(jnp.int32)
        keys.append((1 + near - far) * count + k)
    order = [jnp.int32(0)] * count
    for k in range(count):
        place = sum((keys[j] < keys[k]).astype(jnp.int32) for j in range(count) if j != k)
        order = [jnp.where(place == p, jnp.int32(k), order[p]) for p in range(count)]
    return order


def wait_all(copies):
    for copy in copies:
        copy.wait()


def substitute(off_ref, f, inverse, begin, finish):
    brows, kband = f.shape[0], f.shape[1]
    solved = []
    for i in range(brows):
        rest = begin(i)
        for j in range(i):
            at, found = jnp.int32(0), jnp.bool_(False)
            for band in range(kband):
                same = off_ref[band, 0, i] == i - j
                at = jnp.where(same, jnp.int32(band), at)
                found = jnp.logical_or(found, same)
            block = jnp.where(found, f[i, at], 0.0)
            rest = rest - three(nt, solved[j], *split(block))
        x = three(nt, stacked(rest), *split(inverse[i]))
        solved.append(stacked(x))
        finish(i, x)


def early_kernel(inv_hbm, b_hbm, out, inverse, b, sems):
    @pl.when(lax.axis_index("row") == 0)
    def _():
        copies = [
            pltpu.make_async_copy(b_hbm.at[0, pl.ds(0, inverse.shape[0])], b, sems.at[0]),
            pltpu.make_async_copy(inv_hbm.at[0, 0], inverse, sems.at[1]),
        ]
        for copy in copies:
            copy.start()
        copies[0].wait()
        right = stacked(b[...].T)
        copies[1].wait()
        out[...] = three(nt, right, *split(inverse[...]))


def early_solve(inverses, coupling):
    size, cols = inverses.shape[2], coupling.shape[2]
    hbm = pl.BlockSpec(memory_space=pltpu.HBM)
    return pl.pallas_call(
        early_kernel,
        in_specs=[hbm] * 2,
        out_shape=jax.ShapeDtypeStruct((cols, size), F32),
        scratch_shapes=[
            pltpu.VMEM((size, size), F32),
            pltpu.VMEM((size, cols), F32),
            pltpu.SemaphoreType.DMA((2,)),
        ],
        compiler_params=pltpu.CompilerParams(vmem_limit_bytes=ALONE),
        cost_estimate=pl.CostEstimate(flops=6 * size * size * cols, bytes_accessed=1 << 20, transcendentals=0),
        name="early",
    )(inverses, coupling)


def arrange_kernel(ids_ref, x_ref, out):
    @pl.when(lax.axis_index("row") > 0)
    def _():
        order = ordered(ids_ref, lax.axis_index("sub"))
        tile = x_ref.shape[0] // len(order)
        for p, k in enumerate(order):
            out[p * tile : (p + 1) * tile] = x_ref[pl.ds(pl.multiple_of(k * tile, tile), tile)]


def arrange(ids, x):
    return pl.pallas_call(
        arrange_kernel,
        in_specs=[pl.BlockSpec(memory_space=pltpu.SMEM), pl.BlockSpec(memory_space=pltpu.VMEM)],
        out_shape=jax.ShapeDtypeStruct(x.shape, F32),
        compiler_params=pltpu.CompilerParams(vmem_limit_bytes=VMEM_LIMIT),
        name="arrange",
    )(ids, x)


def solve_kernel(off_ref, ids_ref, f_hbm, inv_hbm, b_hbm, top, *rest, chunks, tiles):
    outs, (f, inverse, b, sems) = rest[: len(chunks)], rest[len(chunks) :]
    brows, _, size, _ = f.shape
    tile = b.shape[2] // tiles

    order = ordered(ids_ref, lax.axis_index("sub"))
    copies = []
    for i in range(brows):
        group = [pltpu.make_async_copy(inv_hbm.at[0, i], inverse.at[i], sems.at[0, i])]
        for p in range(tiles):
            columns = pl.ds(pl.multiple_of(order[p] * tile, tile), tile)
            group.append(
                pltpu.make_async_copy(
                    b_hbm.at[0, pl.ds(i * size, size), columns],
                    b.at[i, :, pl.ds(p * tile, tile)],
                    sems.at[2 + p, i],
                )
            )
        if i > 0:
            group.append(pltpu.make_async_copy(f_hbm.at[0, i], f.at[i], sems.at[1, i]))
        for copy in group:
            copy.start()
        copies.append(group)

    def begin(i):
        wait_all(copies[i])
        return b[i].T

    def finish(i, x):
        if i == 0:
            top[...] = x
            return
        start = 0
        for out, n in zip(outs, chunks):
            out[:, (i - 1) * size : i * size] = x[start : start + n]
            start += n

    substitute(off_ref, f, inverse, begin, finish)


def solve(offsets, ids, blocks, inverses, coupling, chunks, tile):
    _, brows, kband, size, _ = blocks.shape
    total = sum(chunks)
    tiles = total // tile
    hbm = pl.BlockSpec(memory_space=pltpu.HBM)
    smem = pl.BlockSpec(memory_space=pltpu.SMEM)
    return pl.pallas_call(
        functools.partial(solve_kernel, chunks=chunks, tiles=tiles),
        in_specs=[smem, smem, hbm, hbm, hbm],
        out_shape=[jax.ShapeDtypeStruct((total, size), F32)]
        + [jax.ShapeDtypeStruct((n, (brows - 1) * size), F32) for n in chunks],
        scratch_shapes=[
            pltpu.VMEM((brows, kband, size, size), F32),
            pltpu.VMEM((brows, size, size), F32),
            pltpu.VMEM((brows, size, total), F32),
            pltpu.SemaphoreType.DMA((2 + tiles, brows)),
        ],
        compiler_params=pltpu.CompilerParams(vmem_limit_bytes=OTHERS),
        cost_estimate=pl.CostEstimate(flops=6 * 10 * size * size * total, bytes_accessed=8 << 20, transcendentals=0),
        name="others",
    )(offsets, ids, blocks, inverses, coupling)


def response_kernel(off_ref, f_hbm, inv_hbm, gh_ref, gl_ref, f, inverse, acc, sems):
    brows, kband, size, _ = f.shape

    @pl.when(lax.axis_index("row") > 0)
    def _():
        copies = []
        for i in range(brows):
            group = [
                pltpu.make_async_copy(inv_hbm.at[0, i], inverse.at[i], sems.at[0, i]),
                pltpu.make_async_copy(f_hbm.at[0, i], f.at[i], sems.at[1, i]),
            ]
            for copy in group:
                copy.start()
            copies.append(group)

        def begin(i):
            wait_all(copies[i])
            acc[...] = jnp.zeros_like(acc)
            for band in range(kband):
                source = i - off_ref[band, 0, i]

                @pl.when(source < 0)
                def _():
                    at = pl.multiple_of((source + brows) * size, size)
                    acc[pl.ds(at, size), :] += f[i, band].T

            return acc[...]

        def finish(i, x):
            at = slice(i * size, (i + 1) * size)
            gh_ref[:, at], gl_ref[:, at] = split(x)

        substitute(off_ref, f, inverse, begin, finish)


def response(offsets, blocks, inverses):
    _, brows, kband, size, _ = blocks.shape
    width = brows * size
    hbm = pl.BlockSpec(memory_space=pltpu.HBM)
    return pl.pallas_call(
        response_kernel,
        in_specs=[pl.BlockSpec(memory_space=pltpu.SMEM), hbm, hbm],
        out_shape=[jax.ShapeDtypeStruct((width, width), BF16)] * 2,
        scratch_shapes=[
            pltpu.VMEM((brows, kband, size, size), F32),
            pltpu.VMEM((brows, size, size), F32),
            pltpu.VMEM((width, size), F32),
            pltpu.SemaphoreType.DMA((2, brows)),
        ],
        compiler_params=pltpu.CompilerParams(vmem_limit_bytes=VMEM_LIMIT),
        cost_estimate=pl.CostEstimate(flops=6 * 10 * size * size * width, bytes_accessed=8 << 20, transcendentals=0),
        name="response",
    )(offsets, blocks, inverses)


def update_kernel(*refs, chunks, stage):
    gh_ref, gl_ref = refs[:2]
    width = 1 + len(chunks)
    recv, y, cur, out = (refs[2 + k * width : 2 + (k + 1) * width] for k in range(4))
    for source, target in zip(cur, out):
        target[...] = source[...]

    @pl.when(lax.axis_index("row") == stage)
    def _():
        size = recv[0].shape[1]
        start = 0
        for c, n in enumerate(chunks):
            rows = slice(start, start + n)
            given = jnp.concatenate([recv[0][rows], recv[1 + c][...]], axis=1)
            change = three(nn, stacked(given), gh_ref[...], gl_ref[...])
            out[0][rows] = y[0][rows] - change[:, :size]
            out[1 + c][...] = y[1 + c][...] - change[:, size:]
            start += n


def update(recv, y, cur, gain, chunks, stage):
    return pl.pallas_call(
        functools.partial(update_kernel, chunks=chunks, stage=stage),
        out_shape=[jax.ShapeDtypeStruct(x.shape, F32) for x in y],
        compiler_params=pltpu.CompilerParams(vmem_limit_bytes=VMEM_LIMIT),
        name="update",
    )(*gain, *recv, *y, *cur)


def gram_kernel(*refs, start, fused, clear, last, share, tile):
    recv0_ref, recv_ref, y0_ref, y_ref = refs[:4]
    refs = refs[4:]
    if fused:
        gh_ref, gl_ref = refs[:2]
        refs = refs[2:]
    if start:
        oldh_ref, oldl_ref = refs[:2]
        refs = refs[2:]
    piece, rest = refs[0], refs[1:]
    n = recv_ref.shape[0]
    here = slice(start, start + n)

    @pl.when(lax.axis_index("row") > 0)
    def _():
        recv = stacked(jnp.concatenate([recv0_ref[here], recv_ref[...]], axis=1))
        x = jnp.concatenate([y0_ref[here], y_ref[...]], axis=1)
        if fused:
            x = x - three(nn, recv, gh_ref[...], gl_ref[...])
        x = stacked(x)
        high = jnp.concatenate([recv[:n], x[:n]], axis=1)
        low = jnp.concatenate([recv[n:], x[n:]], axis=1)
        both = jnp.concatenate([high, low], axis=0)
        if start:
            piece[:, :start] = three(nn, both, oldh_ref[:, :start], oldl_ref[:, :start])
        piece[:, here] = three(nt, both, high, low)
        if not last:
            rest[0][:, here] = high.T
            rest[1][:, here] = low.T
        elif share:
            rest[0][...] = jnp.concatenate(
                [piece[:, t * tile : t * tile + share] for t in range((start + n) // tile)], axis=1
            )

    if clear:

        @pl.when(lax.axis_index("row") == 0)
        def _():
            piece[...] = jnp.zeros_like(piece)


def gram(recv, y, gain, kept, start, total, tile, share, clear):
    n = recv[1].shape[0]
    half = recv[0].shape[1] + recv[1].shape[1]
    last = start + n == total
    inputs = [*recv, *y, *gain, *kept]
    if not last:
        more = [jax.ShapeDtypeStruct((2 * half, total), BF16)] * 2
    else:
        more = [jax.ShapeDtypeStruct((n, total // tile * share), F32)] if share else []
    results = pl.pallas_call(
        functools.partial(
            gram_kernel, start=start, fused=bool(gain), clear=clear, last=last, share=share, tile=tile
        ),
        in_specs=[pl.BlockSpec(memory_space=pltpu.VMEM)] * len(inputs),
        out_shape=[jax.ShapeDtypeStruct((n, start + n), F32)] + more,
        input_output_aliases={len(inputs) - 2 + i: 1 + i for i in range(2)} if start and not last else {},
        compiler_params=pltpu.CompilerParams(vmem_limit_bytes=VMEM_LIMIT),
        cost_estimate=pl.CostEstimate(
            flops=6 * n * half * (half + 2 * (start + n)), bytes_accessed=4 << 20, transcendentals=0
        ),
    )(*inputs)
    return results[0], list(results[1:])


def fill(out, chunks, part, tile, low_tile):
    share = out.shape[1]
    low, high = part * share, (part + 1) * share
    base = low_tile * tile
    for start, piece in chunks:
        n = piece.shape[0]
        at, inner = start // tile, start % tile
        if piece.shape[1] < start + n:
            turned = piece[:, low_tile * share :].T
            for t in range(low_tile, at + 1):
                first = (t - low_tile) * share
                out[t - low_tile, :, start - base : start - base + n] = turned[first : first + share]
            continue
        first, stop = max(inner, low), min(inner + n, high)
        if first < stop:
            out[at - low_tile, first - low : stop - low, : start + n - base] = piece[first - inner : stop - inner, base:]
        if start > base:
            turned = piece[:, base:start].T
            for t in range(low_tile, -(-start // tile)):
                first, stop = t * tile + low, min(t * tile + high, start)
                if first < stop:
                    out[t - low_tile, : stop - first, start - base : start - base + n] = turned[
                        first - base : stop - base
                    ]


def fill_mine(out, starts, pieces, parts, tile, low_tile):
    row = lax.axis_index("row")
    both = len(pieces) > len(starts)
    for part in range(parts):
        mine = pieces[len(starts) :] if both and part else pieces[: len(starts)]
        pl.when(row == part)(functools.partial(fill, out, list(zip(starts, mine)), part, tile, low_tile))


def pair_kernel(*refs, starts, parts, tile, low_tile):
    fill_mine(refs[-1], starts, refs[:-1], parts, tile, low_tile)


def pair(pieces, starts, parts, tile, share, low_tile):
    return pl.pallas_call(
        functools.partial(pair_kernel, starts=starts, parts=parts, tile=tile, low_tile=low_tile),
        out_shape=jax.ShapeDtypeStruct((PAIR, share, PAIR * tile), F32),
        compiler_params=pltpu.CompilerParams(vmem_limit_bytes=VMEM_LIMIT),
    )(*pieces)


def matches(ids, other, low_tile):
    count, total = ids.shape
    sub = lax.axis_index("sub")
    inside = jnp.logical_and(other >= 0, other < total)
    other = jnp.clip(other, 0, total - 1)
    order = ordered(ids, other)
    slots = []
    for m in range(PAIR):
        number = ids[order[low_tile + m], other]
        place, hit = jnp.int32(0), jnp.bool_(False)
        for i in range(count):
            same = ids[i, sub] == number
            place = jnp.where(same, jnp.int32(i), place)
            hit = jnp.logical_or(hit, same)
        slots.append((place, jnp.logical_and(hit, inside)))
    return slots


def subtract_halo(ids, out, halo, other, low_tile):
    tile = halo.shape[2] // PAIR
    slots = matches(ids, other, low_tile)
    for m in range(PAIR):
        for n in range(PAIR):

            @pl.when(jnp.logical_and(slots[m][1], slots[n][1]))
            def _():
                at = pl.multiple_of(slots[n][0] * tile, tile)
                out[slots[m][0], :, pl.ds(at, tile)] -= halo[m, :, n * tile : (n + 1) * tile]


def subtract_gram(ids_ref, out, g, chunks, parts, tile, blocks):
    starts, pieces = chunks
    for p, q in blocks:
        g[p, :, q * tile : (q + 1) * tile] = jnp.zeros((g.shape[1], tile), F32)
    fill_mine(g, starts, pieces, parts, tile, 0)
    order = ordered(ids_ref, lax.axis_index("sub"))
    for p, q in blocks:
        at = pl.multiple_of(order[q] * tile, tile)
        out[order[p], :, pl.ds(at, tile)] -= g[p, :, q * tile : (q + 1) * tile]


def middle_kernel(ids_ref, face_ref, halo_ref, *refs, starts, parts, tile):
    pieces, (out_ref, g) = refs[:-2], refs[-2:]
    count = out_ref.shape[0]
    out_ref[...] = face_ref[0]
    blocks = [(p, q) for p in range(count) for q in range(count)]
    subtract_gram(ids_ref, out_ref, g, (starts, pieces), parts, tile, blocks)
    subtract_halo(ids_ref, out_ref, halo_ref, far_of(lax.axis_index("sub")), 0)


def rest_kernel(ids_ref, base_ref, *refs, starts, parts, tile, low_tile):
    pieces, (out_ref, weight_ref, g) = refs[:-3], refs[-3:]
    count = out_ref.shape[0]
    last = count - 1
    out_ref[...] = base_ref[...]
    blocks = [(p, q) for p in range(count) for q in range(count) if last in (p, q)]
    subtract_gram(ids_ref, out_ref, g, (starts, pieces), parts, tile, blocks)
    slots = matches(ids_ref, near_of(lax.axis_index("sub")), low_tile)
    for m, (place, hit) in enumerate(slots):
        for i in range(count):
            weight = jnp.logical_and(hit, place == i).astype(F32)
            weight_ref[m, i] = jnp.full(weight_ref.shape[2:], weight, F32)


def finish_kernel(base_ref, halo_ref, weight_ref, out_ref):
    count, _, cols = base_ref.shape
    tile = cols // count
    for i in range(count):
        left = [weight_ref[m, i, 0:1] for m in range(PAIR)]
        for j in range(count):
            right = [weight_ref[n, j, 0:1] for n in range(PAIR)]
            block = base_ref[i, :, j * tile : (j + 1) * tile]
            for m in range(PAIR):
                for n in range(PAIR):
                    block = block - (left[m] * right[n]) * halo_ref[m, :, n * tile : (n + 1) * tile]
            out_ref[i, :, j * tile : (j + 1) * tile] = block


def assemble(kernel, ids, arrays, shapes, scratch):
    smem = pl.BlockSpec(memory_space=pltpu.SMEM)
    vmem = pl.BlockSpec(memory_space=pltpu.VMEM)
    return pl.pallas_call(
        kernel,
        in_specs=[smem] * len(ids) + [vmem] * len(arrays),
        out_shape=[jax.ShapeDtypeStruct(shape, F32) for shape in shapes],
        scratch_shapes=[pltpu.VMEM(scratch, F32)] if scratch else [],
        compiler_params=pltpu.CompilerParams(vmem_limit_bytes=VMEM_LIMIT),
    )(*ids, *arrays)


def sizes(count, tile):
    short = tile * LAST[0] // LAST[1]
    return (tile,) * (count - 1) + (tile - short, short)


def shards(factor_blocks, block_inverses, band_offsets, coupling, interface_block, tile_ids):
    rows = lax.axis_size("row")
    subs = lax.axis_size("sub")
    _, count, share, cols = interface_block.shape
    tile = cols // count
    chunks = sizes(count, tile)
    starts = [sum(chunks[:c]) for c in range(len(chunks))]
    offsets = jnp.transpose(band_offsets, (2, 0, 1))
    ids = jnp.transpose(tile_ids)
    far = [(s, s - 1 + 2 * (s % 2)) for s in range(subs)]
    near = [(s, s + 1 - 2 * (s % 2)) for s in range(subs)]
    far, near = ([(s, t) for s, t in pairs if 0 <= t < subs] for pairs in (far, near))
    early = early_solve(block_inverses, coupling) if rows == 2 else None
    ys = list(solve(offsets, ids, factor_blocks, block_inverses, coupling, chunks, tile))
    gain = response(offsets, factor_blocks, block_inverses)
    xs = [early] + ys[1:] if rows == 2 else ys
    first = None
    for stage in range(1, rows):
        recv = []
        for x in xs:
            recv.append(lax.ppermute(x, "row", [(stage - 1, stage)]))
        if rows == 2:
            recv[0] = arrange(ids, recv[0])
        first = first or recv
        if rows > 2:
            xs = list(update(recv, ys, xs, gain, chunks, stage))
    mine, gain_now = (ys, gain) if rows == 2 else (xs, ())
    kept, own, got = [], [], []
    for c, start in enumerate(starts):
        narrow = share if rows == 2 and start % tile >= share else 0
        piece, kept = gram(
            (first[0], first[1 + c]), (mine[0], mine[1 + c]), gain_now, kept, start, cols, tile, narrow, rows > 2
        )
        if rows == 2:
            got.append(lax.ppermute(kept[0] if narrow else piece, "row", [(1, 0)]))
            own.append(piece)
        else:
            got.append(lax.psum(piece, "row"))
    shape = (count, share, cols)
    last = count - PAIR

    def pick(low, high):
        return got[low:high] + own[low:high]

    message = pair(pick(0, PAIR), starts[:PAIR], rows, tile, share, 0)
    from_far = lax.ppermute(message, "sub", far)
    kernel = functools.partial(middle_kernel, starts=starts[:-1], parts=rows, tile=tile)
    arrays = [interface_block, from_far] + got[:-1] + own[:-1]
    (base,) = assemble(kernel, [ids], arrays, [shape], shape)
    message = pair(pick(last, None), starts[last:], rows, tile, share, last)
    from_near = lax.ppermute(message, "sub", near)
    kernel = functools.partial(rest_kernel, starts=starts[-1:], parts=rows, tile=tile, low_tile=last)
    arrays = [base] + pick(-1, None)
    base, weights = assemble(kernel, [ids], arrays, [shape, (PAIR, count, 8, tile)], shape)
    (out,) = assemble(finish_kernel, [], [base, from_near, weights], [shape], None)
    return out[None]


def solution(mesh):
    return jax.shard_map(
        shards,
        mesh=mesh,
        in_specs=(
            P("sub", "row", None, None, None),
            P("sub", "row", None, None),
            P("sub", "row", None),
            P("sub", "row", None),
            P("sub", None, "row", None),
            P(),
        ),
        out_specs=P("sub", None, "row", None),
        check_vma=False,
    )
```

```python
import functools

import jax
import jax.numpy as jnp
from jax import lax
from jax.experimental import pallas as pl
from jax.experimental.pallas import tpu as pltpu
from jax.sharding import PartitionSpec as P


F32 = jnp.float32
BF16 = jnp.bfloat16
VMEM_LIMIT = 24 * 1024 * 1024
OTHERS = 52 * 1024 * 1024
ALONE = 53 * 1024 * 1024
PAIR = 2
LAST = (1, 2)


def split(x):
    high = x.astype(BF16)
    return high, (x - high.astype(F32)).astype(BF16)


def nt(a, b):
    return lax.dot_general(a, b, (((1,), (1,)), ((), ())), preferred_element_type=F32)


def nn(a, b):
    return lax.dot_general(a, b, (((1,), (0,)), ((), ())), preferred_element_type=F32)


def three(dot, both, high, low):
    rows = both.shape[0] // 2
    wide = dot(both, high)
    return wide[:rows] + (wide[rows:] + dot(both[:rows], low))


def stacked(x):
    return jnp.concatenate(split(x), axis=0)


def near_of(sub):
    return sub + 1 - 2 * (sub % 2)


def far_of(sub):
    return sub - 1 + 2 * (sub % 2)


def shares(ids, k, sub, other):
    count, total = ids.shape
    inside = jnp.logical_and(other >= 0, other < total)
    other = jnp.clip(other, 0, total - 1)
    hit = ids[k, sub] == ids[0, other]
    for i in range(1, count):
        hit = jnp.logical_or(hit, ids[k, sub] == ids[i, other])
    return jnp.logical_and(hit, inside)


def ordered(ids, sub):
    count = ids.shape[0]
    keys = []
    for k in range(count):
        far = shares(ids, k, sub, far_of(sub)).astype(jnp.int32)
        near = shares(ids, k, sub, near_of(sub)).astype(jnp.int32)
        keys.append((1 + near - far) * count + k)
    order = [jnp.int32(0)] * count
    for k in range(count):
        place = sum((keys[j] < keys[k]).astype(jnp.int32) for j in range(count) if j != k)
        order = [jnp.where(place == p, jnp.int32(k), order[p]) for p in range(count)]
    return order


def wait_all(copies):
    for copy in copies:
        copy.wait()


def substitute(off_ref, f, inverse, begin, finish):
    brows, kband = f.shape[0], f.shape[1]
    solved = []
    for i in range(brows):
        rest = begin(i)
        for j in range(i):
            at, found = jnp.int32(0), jnp.bool_(False)
            for band in range(kband):
                same = off_ref[band, 0, i] == i - j
                at = jnp.where(same, jnp.int32(band), at)
                found = jnp.logical_or(found, same)
            block = jnp.where(found, f[i, at], 0.0)
            rest = rest - three(nt, solved[j], *split(block))
        x = three(nt, stacked(rest), *split(inverse[i]))
        solved.append(stacked(x))
        finish(i, x)


def early_kernel(inv_hbm, b_hbm, out, inverse, b, sems):
    @pl.when(lax.axis_index("row") == 0)
    def _():
        copies = [
            pltpu.make_async_copy(b_hbm.at[0, pl.ds(0, inverse.shape[0])], b, sems.at[0]),
            pltpu.make_async_copy(inv_hbm.at[0, 0], inverse, sems.at[1]),
        ]
        for copy in copies:
            copy.start()
        copies[0].wait()
        right = stacked(b[...].T)
        copies[1].wait()
        out[...] = three(nt, right, *split(inverse[...]))


def early_solve(inverses, coupling):
    size, cols = inverses.shape[2], coupling.shape[2]
    hbm = pl.BlockSpec(memory_space=pltpu.HBM)
    return pl.pallas_call(
        early_kernel,
        in_specs=[hbm] * 2,
        out_shape=jax.ShapeDtypeStruct((cols, size), F32),
        scratch_shapes=[
            pltpu.VMEM((size, size), F32),
            pltpu.VMEM((size, cols), F32),
            pltpu.SemaphoreType.DMA((2,)),
        ],
        compiler_params=pltpu.CompilerParams(vmem_limit_bytes=ALONE),
        cost_estimate=pl.CostEstimate(flops=6 * size * size * cols, bytes_accessed=1 << 20, transcendentals=0),
        name="early",
    )(inverses, coupling)


def arrange_kernel(ids_ref, x_ref, out):
    @pl.when(lax.axis_index("row") > 0)
    def _():
        order = ordered(ids_ref, lax.axis_index("sub"))
        tile = x_ref.shape[0] // len(order)
        for p, k in enumerate(order):
            out[p * tile : (p + 1) * tile] = x_ref[pl.ds(pl.multiple_of(k * tile, tile), tile)]


def arrange(ids, x):
    return pl.pallas_call(
        arrange_kernel,
        in_specs=[pl.BlockSpec(memory_space=pltpu.SMEM), pl.BlockSpec(memory_space=pltpu.VMEM)],
        out_shape=jax.ShapeDtypeStruct(x.shape, F32),
        compiler_params=pltpu.CompilerParams(vmem_limit_bytes=VMEM_LIMIT),
        name="arrange",
    )(ids, x)


def solve_kernel(off_ref, ids_ref, f_hbm, inv_hbm, b_hbm, top, *rest, chunks, tiles):
    outs, (f, inverse, b, sems) = rest[: len(chunks)], rest[len(chunks) :]
    brows, _, size, _ = f.shape
    tile = b.shape[2] // tiles

    order = ordered(ids_ref, lax.axis_index("sub"))
    copies = []
    for i in range(brows):
        group = [pltpu.make_async_copy(inv_hbm.at[0, i], inverse.at[i], sems.at[0, i])]
        for p in range(tiles):
            columns = pl.ds(pl.multiple_of(order[p] * tile, tile), tile)
            group.append(
                pltpu.make_async_copy(
                    b_hbm.at[0, pl.ds(i * size, size), columns],
                    b.at[i, :, pl.ds(p * tile, tile)],
                    sems.at[2 + p, i],
                )
            )
        if i > 0:
            group.append(pltpu.make_async_copy(f_hbm.at[0, i], f.at[i], sems.at[1, i]))
        for copy in group:
            copy.start()
        copies.append(group)

    def begin(i):
        wait_all(copies[i])
        return b[i].T

    def finish(i, x):
        if i == 0:
            top[...] = x
            return
        start = 0
        for out, n in zip(outs, chunks):
            out[:, (i - 1) * size : i * size] = x[start : start + n]
            start += n

    substitute(off_ref, f, inverse, begin, finish)


def solve(offsets, ids, blocks, inverses, coupling, chunks, tile):
    _, brows, kband, size, _ = blocks.shape
    total = sum(chunks)
    tiles = total // tile
    hbm = pl.BlockSpec(memory_space=pltpu.HBM)
    smem = pl.BlockSpec(memory_space=pltpu.SMEM)
    return pl.pallas_call(
        functools.partial(solve_kernel, chunks=chunks, tiles=tiles),
        in_specs=[smem, smem, hbm, hbm, hbm],
        out_shape=[jax.ShapeDtypeStruct((total, size), F32)]
        + [jax.ShapeDtypeStruct((n, (brows - 1) * size), F32) for n in chunks],
        scratch_shapes=[
            pltpu.VMEM((brows, kband, size, size), F32),
            pltpu.VMEM((brows, size, size), F32),
            pltpu.VMEM((brows, size, total), F32),
            pltpu.SemaphoreType.DMA((2 + tiles, brows)),
        ],
        compiler_params=pltpu.CompilerParams(vmem_limit_bytes=OTHERS),
        cost_estimate=pl.CostEstimate(flops=6 * 10 * size * size * total, bytes_accessed=8 << 20, transcendentals=0),
        name="others",
    )(offsets, ids, blocks, inverses, coupling)


def response_kernel(off_ref, f_hbm, inv_hbm, gh_ref, gl_ref, f, inverse, acc, sems):
    brows, kband, size, _ = f.shape

    @pl.when(lax.axis_index("row") > 0)
    def _():
        copies = []
        for i in range(brows):
            group = [
                pltpu.make_async_copy(inv_hbm.at[0, i], inverse.at[i], sems.at[0, i]),
                pltpu.make_async_copy(f_hbm.at[0, i], f.at[i], sems.at[1, i]),
            ]
            for copy in group:
                copy.start()
            copies.append(group)

        def begin(i):
            wait_all(copies[i])
            acc[...] = jnp.zeros_like(acc)
            for band in range(kband):
                source = i - off_ref[band, 0, i]

                @pl.when(source < 0)
                def _():
                    at = pl.multiple_of((source + brows) * size, size)
                    acc[pl.ds(at, size), :] += f[i, band].T

            return acc[...]

        def finish(i, x):
            at = slice(i * size, (i + 1) * size)
            gh_ref[:, at], gl_ref[:, at] = split(x)

        substitute(off_ref, f, inverse, begin, finish)


def response(offsets, blocks, inverses):
    _, brows, kband, size, _ = blocks.shape
    width = brows * size
    hbm = pl.BlockSpec(memory_space=pltpu.HBM)
    return pl.pallas_call(
        response_kernel,
        in_specs=[pl.BlockSpec(memory_space=pltpu.SMEM), hbm, hbm],
        out_shape=[jax.ShapeDtypeStruct((width, width), BF16)] * 2,
        scratch_shapes=[
            pltpu.VMEM((brows, kband, size, size), F32),
            pltpu.VMEM((brows, size, size), F32),
            pltpu.VMEM((width, size), F32),
            pltpu.SemaphoreType.DMA((2, brows)),
        ],
        compiler_params=pltpu.CompilerParams(vmem_limit_bytes=VMEM_LIMIT),
        cost_estimate=pl.CostEstimate(flops=6 * 10 * size * size * width, bytes_accessed=8 << 20, transcendentals=0),
        name="response",
    )(offsets, blocks, inverses)


def update_kernel(*refs, chunks, stage):
    gh_ref, gl_ref = refs[:2]
    width = 1 + len(chunks)
    recv, y, cur, out = (refs[2 + k * width : 2 + (k + 1) * width] for k in range(4))
    for source, target in zip(cur, out):
        target[...] = source[...]

    @pl.when(lax.axis_index("row") == stage)
    def _():
        size = recv[0].shape[1]
        start = 0
        for c, n in enumerate(chunks):
            rows = slice(start, start + n)
            given = jnp.concatenate([recv[0][rows], recv[1 + c][...]], axis=1)
            change = three(nn, stacked(given), gh_ref[...], gl_ref[...])
            out[0][rows] = y[0][rows] - change[:, :size]
            out[1 + c][...] = y[1 + c][...] - change[:, size:]
            start += n


def update(recv, y, cur, gain, chunks, stage):
    return pl.pallas_call(
        functools.partial(update_kernel, chunks=chunks, stage=stage),
        out_shape=[jax.ShapeDtypeStruct(x.shape, F32) for x in y],
        compiler_params=pltpu.CompilerParams(vmem_limit_bytes=VMEM_LIMIT),
        name="update",
    )(*gain, *recv, *y, *cur)


def gram_kernel(*refs, start, fused, clear, last, share, tile):
    recv0_ref, recv_ref, y0_ref, y_ref = refs[:4]
    refs = refs[4:]
    if fused:
        gh_ref, gl_ref = refs[:2]
        refs = refs[2:]
    if start:
        oldh_ref, oldl_ref = refs[:2]
        refs = refs[2:]
    piece, rest = refs[0], refs[1:]
    n = recv_ref.shape[0]
    here = slice(start, start + n)
    at, inner = start // tile, start % tile

    @pl.when(lax.axis_index("row") > 0)
    def _():
        recv = stacked(jnp.concatenate([recv0_ref[here], recv_ref[...]], axis=1))
        x = jnp.concatenate([y0_ref[here], y_ref[...]], axis=1)
        if fused:
            x = x - three(nn, recv, gh_ref[...], gl_ref[...])
        x = stacked(x)
        high = jnp.concatenate([recv[:n], x[:n]], axis=1)
        low = jnp.concatenate([recv[n:], x[n:]], axis=1)
        both = jnp.concatenate([high, low], axis=0)
        if share and last:
            middle = oldh_ref.shape[1] // 2
            piece[...] = three(nn, both, oldh_ref[:, :middle], oldl_ref[:, :middle])
            rest[0][...] = both
            return
        if start and share:
            middle = oldh_ref.shape[1] // 2
            stop = middle + at * share
            wide = three(nn, both, oldh_ref[:, :stop], oldl_ref[:, :stop])
            for t in range(at):
                for part in range(2):
                    first = part * middle + t * share
                    left = t * tile + part * share
                    piece[:, left : left + share] = wide[:, first : first + share]
        elif start:
            piece[:, :start] = three(nn, both, oldh_ref[:, :start], oldl_ref[:, :start])
        piece[:, here] = three(nt, both, high, low)
        if last:
            return
        for target, value in zip(rest, (high.T, low.T)):
            if not share:
                target[:, here] = value
                continue
            middle = target.shape[1] // 2
            for part in range(2):
                first, stop = max(inner, part * share), min(inner + n, (part + 1) * share)
                if first < stop:
                    left = part * middle + at * share + first - part * share
                    target[:, left : left + stop - first] = value[:, first - inner : stop - inner]

    if clear:

        @pl.when(lax.axis_index("row") == 0)
        def _():
            piece[...] = jnp.zeros_like(piece)


def gram(recv, y, gain, kept, start, total, tile, share, clear):
    n = recv[1].shape[0]
    half = recv[0].shape[1] + recv[1].shape[1]
    last = start + n == total
    inputs = [*recv, *y, *gain, *kept]
    if last and share:
        shapes = [jax.ShapeDtypeStruct((n, total // 2), F32), jax.ShapeDtypeStruct((2 * n, 2 * half), BF16)]
    else:
        shapes = [jax.ShapeDtypeStruct((n, start + n), F32)]
    if not last:
        shapes += [jax.ShapeDtypeStruct((2 * half, total), BF16)] * 2
    results = pl.pallas_call(
        functools.partial(
            gram_kernel, start=start, fused=bool(gain), clear=clear, last=last, share=share, tile=tile
        ),
        in_specs=[pl.BlockSpec(memory_space=pltpu.VMEM)] * len(inputs),
        out_shape=shapes,
        input_output_aliases={len(inputs) - 2 + i: 1 + i for i in range(2)} if start and not last else {},
        compiler_params=pltpu.CompilerParams(vmem_limit_bytes=VMEM_LIMIT),
        cost_estimate=pl.CostEstimate(
            flops=6 * n * half * (half + 2 * (start + n)), bytes_accessed=4 << 20, transcendentals=0
        ),
    )(*inputs)
    return results[0], list(results[1:])


def widen_kernel(both_ref, oldh_ref, oldl_ref, out):
    n = out.shape[0]
    middle = out.shape[1]
    stop = middle - n

    @pl.when(lax.axis_index("row") > 0)
    def _():
        both = both_ref[...]
        columns = slice(middle, middle + stop)
        out[:, :stop] = three(nn, both, oldh_ref[:, columns], oldl_ref[:, columns])
        out[:, stop:] = three(nt, both, both[:n], both[n:])


def widen(both, kept):
    n, total = both.shape[0] // 2, kept[0].shape[1]
    return pl.pallas_call(
        widen_kernel,
        out_shape=jax.ShapeDtypeStruct((n, total // 2), F32),
        compiler_params=pltpu.CompilerParams(vmem_limit_bytes=VMEM_LIMIT),
        cost_estimate=pl.CostEstimate(flops=6 * n * both.shape[1] * total, bytes_accessed=4 << 20, transcendentals=0),
        name="widen",
    )(both, *kept)


def fill(out, chunks, part, tile, low_tile):
    share = out.shape[1]
    low, high = part * share, (part + 1) * share
    base = low_tile * tile
    for start, piece in chunks:
        if isinstance(piece, tuple):
            narrow, wide = piece
            n, at = narrow.shape[0], start // tile
            for t in range(low_tile, at + 1):
                left, columns = t * tile - base, slice(t * share, (t + 1) * share)
                out[at - low_tile, :, left : left + share] = narrow[:, columns]
                out[at - low_tile, :, left + share : left + tile] = wide[:, columns]
                if t < at:
                    out[t - low_tile, :, start - base : start - base + n] = wide[:, columns].T
            continue
        n = piece.shape[0]
        at, inner = start // tile, start % tile
        if piece.shape[1] < start + n:
            turned = piece[:, low_tile * share :].T
            for t in range(low_tile, at + 1):
                first = (t - low_tile) * share
                out[t - low_tile, :, start - base : start - base + n] = turned[first : first + share]
            continue
        first, stop = max(inner, low), min(inner + n, high)
        if first < stop:
            out[at - low_tile, first - low : stop - low, : start + n - base] = piece[first - inner : stop - inner, base:]
        if start > base:
            turned = piece[:, base:start].T
            for t in range(low_tile, -(-start // tile)):
                first, stop = t * tile + low, min(t * tile + high, start)
                if first < stop:
                    out[t - low_tile, : stop - first, start - base : start - base + n] = turned[
                        first - base : stop - base
                    ]


def fill_mine(out, starts, pieces, parts, tile, low_tile):
    row = lax.axis_index("row")
    both = len(pieces) > len(starts)
    for part in range(parts):
        mine = list(pieces[len(starts) :] if both and part else pieces[: len(starts)])
        if len(mine) > len(starts):
            mine[-2:] = [tuple(mine[-2:])]
        pl.when(row == part)(functools.partial(fill, out, list(zip(starts, mine)), part, tile, low_tile))


def pair_kernel(*refs, starts, parts, tile, low_tile):
    fill_mine(refs[-1], starts, refs[:-1], parts, tile, low_tile)


def pair(pieces, starts, parts, tile, share, low_tile):
    return pl.pallas_call(
        functools.partial(pair_kernel, starts=starts, parts=parts, tile=tile, low_tile=low_tile),
        out_shape=jax.ShapeDtypeStruct((PAIR, share, PAIR * tile), F32),
        compiler_params=pltpu.CompilerParams(vmem_limit_bytes=VMEM_LIMIT),
    )(*pieces)


def matches(ids, other, low_tile):
    count, total = ids.shape
    sub = lax.axis_index("sub")
    inside = jnp.logical_and(other >= 0, other < total)
    other = jnp.clip(other, 0, total - 1)
    order = ordered(ids, other)
    slots = []
    for m in range(PAIR):
        number = ids[order[low_tile + m], other]
        place, hit = jnp.int32(0), jnp.bool_(False)
        for i in range(count):
            same = ids[i, sub] == number
            place = jnp.where(same, jnp.int32(i), place)
            hit = jnp.logical_or(hit, same)
        slots.append((place, jnp.logical_and(hit, inside)))
    return slots


def subtract_halo(ids, out, halo, other, low_tile):
    tile = halo.shape[2] // PAIR
    slots = matches(ids, other, low_tile)
    for m in range(PAIR):
        for n in range(PAIR):

            @pl.when(jnp.logical_and(slots[m][1], slots[n][1]))
            def _():
                at = pl.multiple_of(slots[n][0] * tile, tile)
                out[slots[m][0], :, pl.ds(at, tile)] -= halo[m, :, n * tile : (n + 1) * tile]


def subtract_gram(ids_ref, out, g, chunks, parts, tile, blocks):
    starts, pieces = chunks
    for p, q in blocks:
        g[p, :, q * tile : (q + 1) * tile] = jnp.zeros((g.shape[1], tile), F32)
    fill_mine(g, starts, pieces, parts, tile, 0)
    order = ordered(ids_ref, lax.axis_index("sub"))
    for p, q in blocks:
        at = pl.multiple_of(order[q] * tile, tile)
        out[order[p], :, pl.ds(at, tile)] -= g[p, :, q * tile : (q + 1) * tile]


def middle_kernel(ids_ref, face_ref, halo_ref, *refs, starts, parts, tile):
    pieces, (out_ref, g) = refs[:-2], refs[-2:]
    count = out_ref.shape[0]
    out_ref[...] = face_ref[0]
    blocks = [(p, q) for p in range(count) for q in range(count)]
    subtract_gram(ids_ref, out_ref, g, (starts, pieces), parts, tile, blocks)
    subtract_halo(ids_ref, out_ref, halo_ref, far_of(lax.axis_index("sub")), 0)


def rest_kernel(ids_ref, base_ref, *refs, starts, parts, tile, low_tile):
    pieces, (out_ref, weight_ref, g) = refs[:-3], refs[-3:]
    count = out_ref.shape[0]
    last = count - 1
    out_ref[...] = base_ref[...]
    blocks = [(p, q) for p in range(count) for q in range(count) if last in (p, q)]
    subtract_gram(ids_ref, out_ref, g, (starts, pieces), parts, tile, blocks)
    slots = matches(ids_ref, near_of(lax.axis_index("sub")), low_tile)
    for m, (place, hit) in enumerate(slots):
        for i in range(count):
            weight = jnp.logical_and(hit, place == i).astype(F32)
            weight_ref[m, i] = jnp.full(weight_ref.shape[2:], weight, F32)


def finish_kernel(base_ref, halo_ref, weight_ref, out_ref):
    count, _, cols = base_ref.shape
    tile = cols // count
    for i in range(count):
        left = [weight_ref[m, i, 0:1] for m in range(PAIR)]
        for j in range(count):
            right = [weight_ref[n, j, 0:1] for n in range(PAIR)]
            block = base_ref[i, :, j * tile : (j + 1) * tile]
            for m in range(PAIR):
                for n in range(PAIR):
                    block = block - (left[m] * right[n]) * halo_ref[m, :, n * tile : (n + 1) * tile]
            out_ref[i, :, j * tile : (j + 1) * tile] = block


def assemble(kernel, ids, arrays, shapes, scratch):
    smem = pl.BlockSpec(memory_space=pltpu.SMEM)
    vmem = pl.BlockSpec(memory_space=pltpu.VMEM)
    return pl.pallas_call(
        kernel,
        in_specs=[smem] * len(ids) + [vmem] * len(arrays),
        out_shape=[jax.ShapeDtypeStruct(shape, F32) for shape in shapes],
        scratch_shapes=[pltpu.VMEM(scratch, F32)] if scratch else [],
        compiler_params=pltpu.CompilerParams(vmem_limit_bytes=VMEM_LIMIT),
    )(*ids, *arrays)


def sizes(count, tile):
    short = tile * LAST[0] // LAST[1]
    return (tile,) * (count - 1) + (tile - short, short)


def shards(factor_blocks, block_inverses, band_offsets, coupling, interface_block, tile_ids):
    rows = lax.axis_size("row")
    subs = lax.axis_size("sub")
    _, count, share, cols = interface_block.shape
    tile = cols // count
    chunks = sizes(count, tile)
    starts = [sum(chunks[:c]) for c in range(len(chunks))]
    offsets = jnp.transpose(band_offsets, (2, 0, 1))
    ids = jnp.transpose(tile_ids)
    far = [(s, s - 1 + 2 * (s % 2)) for s in range(subs)]
    near = [(s, s + 1 - 2 * (s % 2)) for s in range(subs)]
    far, near = ([(s, t) for s, t in pairs if 0 <= t < subs] for pairs in (far, near))
    early = early_solve(block_inverses, coupling) if rows == 2 else None
    ys = list(solve(offsets, ids, factor_blocks, block_inverses, coupling, chunks, tile))
    gain = response(offsets, factor_blocks, block_inverses)
    xs = [early] + ys[1:] if rows == 2 else ys
    first = None
    for stage in range(1, rows):
        recv = []
        for x in xs:
            recv.append(lax.ppermute(x, "row", [(stage - 1, stage)]))
        if rows == 2:
            recv[0] = arrange(ids, recv[0])
        first = first or recv
        if rows > 2:
            xs = list(update(recv, ys, xs, gain, chunks, stage))
    mine, gain_now = (ys, gain) if rows == 2 else (xs, ())
    kept, own, got = [], [], []
    halves = share if rows == 2 and all(s % tile in (0, share) for s in starts) else 0
    for c, start in enumerate(starts):
        before = kept
        piece, kept = gram(
            (first[0], first[1 + c]), (mine[0], mine[1 + c]), gain_now, kept, start, cols, tile, halves, rows > 2
        )
        if rows > 2:
            got.append(lax.psum(piece, "row"))
            continue
        got.append(lax.ppermute(piece, "row", [(1, 0)]))
        own.append([piece])
    if halves:
        own[-1].append(widen(kept[0], before))
    shape = (count, share, cols)
    last = count - PAIR

    def pick(low, high):
        return got[low:high] + [x for pieces in own[low:high] for x in pieces]

    message = pair(pick(0, PAIR), starts[:PAIR], rows, tile, share, 0)
    from_far = lax.ppermute(message, "sub", far)
    kernel = functools.partial(middle_kernel, starts=starts[:-1], parts=rows, tile=tile)
    arrays = [interface_block, from_far] + pick(0, -1)
    (base,) = assemble(kernel, [ids], arrays, [shape], shape)
    message = pair(pick(last, None), starts[last:], rows, tile, share, last)
    from_near = lax.ppermute(message, "sub", near)
    kernel = functools.partial(rest_kernel, starts=starts[-1:], parts=rows, tile=tile, low_tile=last)
    arrays = [base] + pick(-1, None)
    base, weights = assemble(kernel, [ids], arrays, [shape, (PAIR, count, 8, tile)], shape)
    (out,) = assemble(finish_kernel, [], [base, from_near, weights], [shape], None)
    return out[None]


def solution(mesh):
    return jax.shard_map(
        shards,
        mesh=mesh,
        in_specs=(
            P("sub", "row", None, None, None),
            P("sub", "row", None, None),
            P("sub", "row", None),
            P("sub", "row", None),
            P("sub", None, "row", None),
            P(),
        ),
        out_specs=P("sub", None, "row", None),
        check_vma=False,
    )
```

```python
import functools

import jax
import jax.numpy as jnp
from jax import lax
from jax.experimental import pallas as pl
from jax.experimental.pallas import tpu as pltpu
from jax.sharding import PartitionSpec as P


F32 = jnp.float32
BF16 = jnp.bfloat16
VMEM_LIMIT = 24 * 1024 * 1024
OTHERS = 52 * 1024 * 1024
ALONE = 53 * 1024 * 1024
PAIR = 2
LAST = (1, 2)


def split(x):
    high = x.astype(BF16)
    return high, (x - high.astype(F32)).astype(BF16)


def nt(a, b):
    return lax.dot_general(a, b, (((1,), (1,)), ((), ())), preferred_element_type=F32)


def nn(a, b):
    return lax.dot_general(a, b, (((1,), (0,)), ((), ())), preferred_element_type=F32)


def three(dot, both, high, low):
    rows = both.shape[0] // 2
    wide = dot(both, high)
    return wide[:rows] + (wide[rows:] + dot(both[:rows], low))


def stacked(x):
    return jnp.concatenate(split(x), axis=0)


def near_of(sub):
    return sub + 1 - 2 * (sub % 2)


def far_of(sub):
    return sub - 1 + 2 * (sub % 2)


def shares(ids, k, sub, other):
    count, total = ids.shape
    inside = jnp.logical_and(other >= 0, other < total)
    other = jnp.clip(other, 0, total - 1)
    hit = ids[k, sub] == ids[0, other]
    for i in range(1, count):
        hit = jnp.logical_or(hit, ids[k, sub] == ids[i, other])
    return jnp.logical_and(hit, inside)


def ordered(ids, sub):
    count = ids.shape[0]
    keys = []
    for k in range(count):
        far = shares(ids, k, sub, far_of(sub)).astype(jnp.int32)
        near = shares(ids, k, sub, near_of(sub)).astype(jnp.int32)
        keys.append((1 + near - far) * count + k)
    order = [jnp.int32(0)] * count
    for k in range(count):
        place = sum((keys[j] < keys[k]).astype(jnp.int32) for j in range(count) if j != k)
        order = [jnp.where(place == p, jnp.int32(k), order[p]) for p in range(count)]
    return order


def wait_all(copies):
    for copy in copies:
        copy.wait()


def substitute(off_ref, f, inverse, begin, finish):
    brows, kband = f.shape[0], f.shape[1]
    solved = []
    for i in range(brows):
        rest = begin(i)
        for j in range(i):
            at, found = jnp.int32(0), jnp.bool_(False)
            for band in range(kband):
                same = off_ref[band, 0, i] == i - j
                at = jnp.where(same, jnp.int32(band), at)
                found = jnp.logical_or(found, same)
            block = jnp.where(found, f[i, at], 0.0)
            rest = rest - three(nt, solved[j], *split(block))
        x = three(nt, stacked(rest), *split(inverse[i]))
        solved.append(stacked(x))
        finish(i, x)


def early_kernel(inv_hbm, b_hbm, out, inverse, b, sems):
    @pl.when(lax.axis_index("row") == 0)
    def _():
        copies = [
            pltpu.make_async_copy(b_hbm.at[0, pl.ds(0, inverse.shape[0])], b, sems.at[0]),
            pltpu.make_async_copy(inv_hbm.at[0, 0], inverse, sems.at[1]),
        ]
        for copy in copies:
            copy.start()
        copies[0].wait()
        right = stacked(b[...].T)
        copies[1].wait()
        out[...] = three(nt, right, *split(inverse[...]))


def early_solve(inverses, coupling):
    size, cols = inverses.shape[2], coupling.shape[2]
    hbm = pl.BlockSpec(memory_space=pltpu.HBM)
    return pl.pallas_call(
        early_kernel,
        in_specs=[hbm] * 2,
        out_shape=jax.ShapeDtypeStruct((cols, size), F32),
        scratch_shapes=[
            pltpu.VMEM((size, size), F32),
            pltpu.VMEM((size, cols), F32),
            pltpu.SemaphoreType.DMA((2,)),
        ],
        compiler_params=pltpu.CompilerParams(vmem_limit_bytes=ALONE),
        cost_estimate=pl.CostEstimate(flops=6 * size * size * cols, bytes_accessed=1 << 20, transcendentals=0),
        name="early",
    )(inverses, coupling)


def arrange_kernel(ids_ref, x_ref, out):
    @pl.when(lax.axis_index("row") > 0)
    def _():
        order = ordered(ids_ref, lax.axis_index("sub"))
        tile = x_ref.shape[0] // len(order)
        for p, k in enumerate(order):
            out[p * tile : (p + 1) * tile] = x_ref[pl.ds(pl.multiple_of(k * tile, tile), tile)]


def arrange(ids, x):
    return pl.pallas_call(
        arrange_kernel,
        in_specs=[pl.BlockSpec(memory_space=pltpu.SMEM), pl.BlockSpec(memory_space=pltpu.VMEM)],
        out_shape=jax.ShapeDtypeStruct(x.shape, F32),
        compiler_params=pltpu.CompilerParams(vmem_limit_bytes=VMEM_LIMIT),
        name="arrange",
    )(ids, x)


def solve_kernel(off_ref, ids_ref, f_hbm, inv_hbm, b_hbm, top, *rest, chunks, tiles):
    outs, (f, inverse, b, sems) = rest[: len(chunks)], rest[len(chunks) :]
    brows, _, size, _ = f.shape
    tile = b.shape[2] // tiles

    order = ordered(ids_ref, lax.axis_index("sub"))
    copies = []
    for i in range(brows):
        group = [pltpu.make_async_copy(inv_hbm.at[0, i], inverse.at[i], sems.at[0, i])]
        for p in range(tiles):
            columns = pl.ds(pl.multiple_of(order[p] * tile, tile), tile)
            group.append(
                pltpu.make_async_copy(
                    b_hbm.at[0, pl.ds(i * size, size), columns],
                    b.at[i, :, pl.ds(p * tile, tile)],
                    sems.at[2 + p, i],
                )
            )
        if i > 0:
            group.append(pltpu.make_async_copy(f_hbm.at[0, i], f.at[i], sems.at[1, i]))
        for copy in group:
            copy.start()
        copies.append(group)

    def begin(i):
        wait_all(copies[i])
        return b[i].T

    def finish(i, x):
        if i == 0:
            top[...] = x
            return
        start = 0
        for out, n in zip(outs, chunks):
            out[:, (i - 1) * size : i * size] = x[start : start + n]
            start += n

    substitute(off_ref, f, inverse, begin, finish)


def solve(offsets, ids, blocks, inverses, coupling, chunks, tile):
    _, brows, kband, size, _ = blocks.shape
    total = sum(chunks)
    tiles = total // tile
    hbm = pl.BlockSpec(memory_space=pltpu.HBM)
    smem = pl.BlockSpec(memory_space=pltpu.SMEM)
    return pl.pallas_call(
        functools.partial(solve_kernel, chunks=chunks, tiles=tiles),
        in_specs=[smem, smem, hbm, hbm, hbm],
        out_shape=[jax.ShapeDtypeStruct((total, size), F32)]
        + [jax.ShapeDtypeStruct((n, (brows - 1) * size), F32) for n in chunks],
        scratch_shapes=[
            pltpu.VMEM((brows, kband, size, size), F32),
            pltpu.VMEM((brows, size, size), F32),
            pltpu.VMEM((brows, size, total), F32),
            pltpu.SemaphoreType.DMA((2 + tiles, brows)),
        ],
        compiler_params=pltpu.CompilerParams(vmem_limit_bytes=OTHERS),
        cost_estimate=pl.CostEstimate(flops=6 * 10 * size * size * total, bytes_accessed=8 << 20, transcendentals=0),
        name="others",
    )(offsets, ids, blocks, inverses, coupling)


def response_kernel(off_ref, f_hbm, inv_hbm, gh_ref, gl_ref, f, inverse, acc, sems):
    brows, kband, size, _ = f.shape

    @pl.when(lax.axis_index("row") > 0)
    def _():
        copies = []
        for i in range(brows):
            group = [
                pltpu.make_async_copy(inv_hbm.at[0, i], inverse.at[i], sems.at[0, i]),
                pltpu.make_async_copy(f_hbm.at[0, i], f.at[i], sems.at[1, i]),
            ]
            for copy in group:
                copy.start()
            copies.append(group)

        def begin(i):
            wait_all(copies[i])
            acc[...] = jnp.zeros_like(acc)
            for band in range(kband):
                source = i - off_ref[band, 0, i]

                @pl.when(source < 0)
                def _():
                    at = pl.multiple_of((source + brows) * size, size)
                    acc[pl.ds(at, size), :] += f[i, band].T

            return acc[...]

        def finish(i, x):
            at = slice(i * size, (i + 1) * size)
            gh_ref[:, at], gl_ref[:, at] = split(x)

        substitute(off_ref, f, inverse, begin, finish)


def response(offsets, blocks, inverses):
    _, brows, kband, size, _ = blocks.shape
    width = brows * size
    hbm = pl.BlockSpec(memory_space=pltpu.HBM)
    return pl.pallas_call(
        response_kernel,
        in_specs=[pl.BlockSpec(memory_space=pltpu.SMEM), hbm, hbm],
        out_shape=[jax.ShapeDtypeStruct((width, width), BF16)] * 2,
        scratch_shapes=[
            pltpu.VMEM((brows, kband, size, size), F32),
            pltpu.VMEM((brows, size, size), F32),
            pltpu.VMEM((width, size), F32),
            pltpu.SemaphoreType.DMA((2, brows)),
        ],
        compiler_params=pltpu.CompilerParams(vmem_limit_bytes=VMEM_LIMIT),
        cost_estimate=pl.CostEstimate(flops=6 * 10 * size * size * width, bytes_accessed=8 << 20, transcendentals=0),
        name="response",
    )(offsets, blocks, inverses)


def update_kernel(*refs, chunks, stage):
    gh_ref, gl_ref = refs[:2]
    width = 1 + len(chunks)
    recv, y, cur, out = (refs[2 + k * width : 2 + (k + 1) * width] for k in range(4))
    for source, target in zip(cur, out):
        target[...] = source[...]

    @pl.when(lax.axis_index("row") == stage)
    def _():
        size = recv[0].shape[1]
        start = 0
        for c, n in enumerate(chunks):
            rows = slice(start, start + n)
            given = jnp.concatenate([recv[0][rows], recv[1 + c][...]], axis=1)
            change = three(nn, stacked(given), gh_ref[...], gl_ref[...])
            out[0][rows] = y[0][rows] - change[:, :size]
            out[1 + c][...] = y[1 + c][...] - change[:, size:]
            start += n


def update(recv, y, cur, gain, chunks, stage):
    return pl.pallas_call(
        functools.partial(update_kernel, chunks=chunks, stage=stage),
        out_shape=[jax.ShapeDtypeStruct(x.shape, F32) for x in y],
        compiler_params=pltpu.CompilerParams(vmem_limit_bytes=VMEM_LIMIT),
        name="update",
    )(*gain, *recv, *y, *cur)


def slot_of(tile, count):
    swapped = {count - 2: count - 1, count - 1: count - 2} if count % 2 == 0 else {}
    return swapped.get(tile, tile)


def gram_kernel(*refs, start, fused, clear, last, share, tile):
    recv0_ref, recv_ref, y0_ref, y_ref = refs[:4]
    refs = refs[4:]
    if fused:
        gh_ref, gl_ref = refs[:2]
        refs = refs[2:]
    if start:
        oldh_ref, oldl_ref = refs[:2]
        refs = refs[2 if last or not share else 4 :]
    piece, rest = refs[0], refs[1:]
    n = recv_ref.shape[0]
    here = slice(start, start + n)

    @pl.when(lax.axis_index("row") > 0)
    def _():
        recv = stacked(jnp.concatenate([recv0_ref[here], recv_ref[...]], axis=1))
        x = jnp.concatenate([y0_ref[here], y_ref[...]], axis=1)
        if fused:
            x = x - three(nn, recv, gh_ref[...], gl_ref[...])
        x = stacked(x)
        high = jnp.concatenate([recv[:n], x[:n]], axis=1)
        low = jnp.concatenate([recv[n:], x[n:]], axis=1)
        both = jnp.concatenate([high, low], axis=0)
        if share and last:
            piece[...] = three(nn, both, oldh_ref[...], oldl_ref[...])
            rest[0][...] = both
            return
        if start:
            piece[:, :start] = three(nn, both, oldh_ref[:, :start], oldl_ref[:, :start])
        piece[:, here] = three(nt, both, high, low)
        if last:
            return
        turned = high.T, low.T
        rest[0][:, here], rest[1][:, here] = turned
        if share:
            left = slot_of(start // tile, rest[0].shape[1] // tile) * share
            columns = slice(left, left + share)
            rest[2][:, columns], rest[3][:, columns] = turned[0][:, :share], turned[1][:, :share]

    if clear:

        @pl.when(lax.axis_index("row") == 0)
        def _():
            piece[...] = jnp.zeros_like(piece)


def gram(recv, y, gain, kept, start, total, tile, share, clear):
    n = recv[1].shape[0]
    half = recv[0].shape[1] + recv[1].shape[1]
    last = start + n == total
    slim = total // tile * share
    if last and share:
        kept = kept[2:]
        shapes = [jax.ShapeDtypeStruct((n, slim), F32), jax.ShapeDtypeStruct((2 * n, 2 * half), BF16)]
    else:
        shapes = [jax.ShapeDtypeStruct((n, start + n), F32)]
    if not last:
        shapes += [jax.ShapeDtypeStruct((2 * half, total), BF16)] * 2
        shapes += [jax.ShapeDtypeStruct((2 * half, slim), BF16)] * 2 if share else []
    inputs = [*recv, *y, *gain, *kept]
    first = len(inputs) - len(kept)
    results = pl.pallas_call(
        functools.partial(
            gram_kernel, start=start, fused=bool(gain), clear=clear, last=last, share=share, tile=tile
        ),
        in_specs=[pl.BlockSpec(memory_space=pltpu.VMEM)] * len(inputs),
        out_shape=shapes,
        input_output_aliases={} if last else {first + i: 1 + i for i in range(len(kept))},
        compiler_params=pltpu.CompilerParams(vmem_limit_bytes=VMEM_LIMIT),
        cost_estimate=pl.CostEstimate(
            flops=6 * n * half * (half + 2 * (start + n)), bytes_accessed=4 << 20, transcendentals=0
        ),
    )(*inputs)
    return results[0], list(results[1:])


def widen_kernel(both_ref, oldh_ref, oldl_ref, out):
    n, total = out.shape
    start = total - n

    @pl.when(lax.axis_index("row") > 0)
    def _():
        both = both_ref[...]
        out[:, :start] = three(nn, both, oldh_ref[:, :start], oldl_ref[:, :start])
        out[:, start:] = three(nt, both, both[:n], both[n:])


def widen(both, kept):
    n, total = both.shape[0] // 2, kept[0].shape[1]
    return pl.pallas_call(
        widen_kernel,
        out_shape=jax.ShapeDtypeStruct((n, total), F32),
        compiler_params=pltpu.CompilerParams(vmem_limit_bytes=VMEM_LIMIT),
        cost_estimate=pl.CostEstimate(flops=6 * n * both.shape[1] * total, bytes_accessed=4 << 20, transcendentals=0),
        name="widen",
    )(both, *kept)


def fill(out, chunks, part, tile, low_tile):
    share = out.shape[1]
    low, high = part * share, (part + 1) * share
    base = low_tile * tile
    for start, piece in chunks:
        n = piece.shape[0]
        at, inner = start // tile, start % tile
        if piece.shape[1] < start + n:
            turned = piece[...].T
            for t in range(low_tile, at + 1):
                first = slot_of(t, at + 1) * share
                out[t - low_tile, :, start - base : start - base + n] = turned[first : first + share]
            continue
        first, stop = max(inner, low), min(inner + n, high)
        if first < stop:
            out[at - low_tile, first - low : stop - low, : start + n - base] = piece[first - inner : stop - inner, base:]
        if start > base:
            turned = piece[:, base:start].T
            for t in range(low_tile, -(-start // tile)):
                first, stop = t * tile + low, min(t * tile + high, start)
                if first < stop:
                    out[t - low_tile, : stop - first, start - base : start - base + n] = turned[
                        first - base : stop - base
                    ]


def fill_mine(out, starts, pieces, parts, tile, low_tile):
    row = lax.axis_index("row")
    both = len(pieces) > len(starts)
    for part in range(parts):
        mine = pieces[len(starts) :] if both and part else pieces[: len(starts)]
        pl.when(row == part)(functools.partial(fill, out, list(zip(starts, mine)), part, tile, low_tile))


def pair_kernel(*refs, starts, parts, tile, low_tile):
    fill_mine(refs[-1], starts, refs[:-1], parts, tile, low_tile)


def pair(pieces, starts, parts, tile, share, low_tile):
    return pl.pallas_call(
        functools.partial(pair_kernel, starts=starts, parts=parts, tile=tile, low_tile=low_tile),
        out_shape=jax.ShapeDtypeStruct((PAIR, share, PAIR * tile), F32),
        compiler_params=pltpu.CompilerParams(vmem_limit_bytes=VMEM_LIMIT),
    )(*pieces)


def matches(ids, other, low_tile):
    count, total = ids.shape
    sub = lax.axis_index("sub")
    inside = jnp.logical_and(other >= 0, other < total)
    other = jnp.clip(other, 0, total - 1)
    order = ordered(ids, other)
    slots = []
    for m in range(PAIR):
        number = ids[order[low_tile + m], other]
        place, hit = jnp.int32(0), jnp.bool_(False)
        for i in range(count):
            same = ids[i, sub] == number
            place = jnp.where(same, jnp.int32(i), place)
            hit = jnp.logical_or(hit, same)
        slots.append((place, jnp.logical_and(hit, inside)))
    return slots


def subtract_halo(ids, out, halo, other, low_tile):
    tile = halo.shape[2] // PAIR
    slots = matches(ids, other, low_tile)
    for m in range(PAIR):
        for n in range(PAIR):

            @pl.when(jnp.logical_and(slots[m][1], slots[n][1]))
            def _():
                at = pl.multiple_of(slots[n][0] * tile, tile)
                out[slots[m][0], :, pl.ds(at, tile)] -= halo[m, :, n * tile : (n + 1) * tile]


def subtract_gram(ids_ref, out, g, chunks, parts, tile, blocks):
    starts, pieces = chunks
    for p, q in blocks:
        g[p, :, q * tile : (q + 1) * tile] = jnp.zeros((g.shape[1], tile), F32)
    fill_mine(g, starts, pieces, parts, tile, 0)
    order = ordered(ids_ref, lax.axis_index("sub"))
    for p, q in blocks:
        at = pl.multiple_of(order[q] * tile, tile)
        out[order[p], :, pl.ds(at, tile)] -= g[p, :, q * tile : (q + 1) * tile]


def middle_kernel(ids_ref, face_ref, halo_ref, *refs, starts, parts, tile):
    pieces, (out_ref, g) = refs[:-2], refs[-2:]
    count = out_ref.shape[0]
    out_ref[...] = face_ref[0]
    blocks = [(p, q) for p in range(count) for q in range(count)]
    subtract_gram(ids_ref, out_ref, g, (starts, pieces), parts, tile, blocks)
    subtract_halo(ids_ref, out_ref, halo_ref, far_of(lax.axis_index("sub")), 0)


def rest_kernel(ids_ref, base_ref, *refs, starts, parts, tile, low_tile):
    pieces, (out_ref, weight_ref, g) = refs[:-3], refs[-3:]
    count = out_ref.shape[0]
    last = count - 1
    out_ref[...] = base_ref[...]
    blocks = [(p, q) for p in range(count) for q in range(count) if last in (p, q)]
    subtract_gram(ids_ref, out_ref, g, (starts, pieces), parts, tile, blocks)
    slots = matches(ids_ref, near_of(lax.axis_index("sub")), low_tile)
    for m, (place, hit) in enumerate(slots):
        for i in range(count):
            weight = jnp.logical_and(hit, place == i).astype(F32)
            weight_ref[m, i] = jnp.full(weight_ref.shape[2:], weight, F32)


def finish_kernel(base_ref, halo_ref, weight_ref, out_ref):
    count, _, cols = base_ref.shape
    tile = cols // count
    for i in range(count):
        left = [weight_ref[m, i, 0:1] for m in range(PAIR)]
        for j in range(count):
            right = [weight_ref[n, j, 0:1] for n in range(PAIR)]
            block = base_ref[i, :, j * tile : (j + 1) * tile]
            for m in range(PAIR):
                for n in range(PAIR):
                    block = block - (left[m] * right[n]) * halo_ref[m, :, n * tile : (n + 1) * tile]
            out_ref[i, :, j * tile : (j + 1) * tile] = block


def assemble(kernel, ids, arrays, shapes, scratch):
    smem = pl.BlockSpec(memory_space=pltpu.SMEM)
    vmem = pl.BlockSpec(memory_space=pltpu.VMEM)
    return pl.pallas_call(
        kernel,
        in_specs=[smem] * len(ids) + [vmem] * len(arrays),
        out_shape=[jax.ShapeDtypeStruct(shape, F32) for shape in shapes],
        scratch_shapes=[pltpu.VMEM(scratch, F32)] if scratch else [],
        compiler_params=pltpu.CompilerParams(vmem_limit_bytes=VMEM_LIMIT),
    )(*ids, *arrays)


def sizes(count, tile):
    short = tile * LAST[0] // LAST[1]
    return (tile,) * (count - 1) + (tile - short, short)


def shards(factor_blocks, block_inverses, band_offsets, coupling, interface_block, tile_ids):
    rows = lax.axis_size("row")
    subs = lax.axis_size("sub")
    _, count, share, cols = interface_block.shape
    tile = cols // count
    chunks = sizes(count, tile)
    starts = [sum(chunks[:c]) for c in range(len(chunks))]
    offsets = jnp.transpose(band_offsets, (2, 0, 1))
    ids = jnp.transpose(tile_ids)
    far = [(s, s - 1 + 2 * (s % 2)) for s in range(subs)]
    near = [(s, s + 1 - 2 * (s % 2)) for s in range(subs)]
    far, near = ([(s, t) for s, t in pairs if 0 <= t < subs] for pairs in (far, near))
    early = early_solve(block_inverses, coupling) if rows == 2 else None
    ys = list(solve(offsets, ids, factor_blocks, block_inverses, coupling, chunks, tile))
    gain = response(offsets, factor_blocks, block_inverses)
    xs = [early] + ys[1:] if rows == 2 else ys
    first = None
    for stage in range(1, rows):
        recv = []
        for x in xs:
            recv.append(lax.ppermute(x, "row", [(stage - 1, stage)]))
        if rows == 2:
            recv[0] = arrange(ids, recv[0])
        first = first or recv
        if rows > 2:
            xs = list(update(recv, ys, xs, gain, chunks, stage))
    mine, gain_now = (ys, gain) if rows == 2 else (xs, ())
    kept, own, got = [], [], []
    slim = share if rows == 2 and all(s % tile in (0, share) for s in starts) else 0
    for c, start in enumerate(starts):
        before = kept
        piece, kept = gram(
            (first[0], first[1 + c]), (mine[0], mine[1 + c]), gain_now, kept, start, cols, tile, slim, rows > 2
        )
        if rows > 2:
            got.append(lax.psum(piece, "row"))
            continue
        got.append(lax.ppermute(piece, "row", [(1, 0)]))
        own.append(piece)
    if slim:
        own[-1] = widen(kept[0], before[:2])
    shape = (count, share, cols)
    last = count - PAIR

    def pick(low, high):
        return got[low:high] + own[low:high]

    message = pair(pick(0, PAIR), starts[:PAIR], rows, tile, share, 0)
    from_far = lax.ppermute(message, "sub", far)
    kernel = functools.partial(middle_kernel, starts=starts[:-1], parts=rows, tile=tile)
    arrays = [interface_block, from_far] + got[:-1] + own[:-1]
    (base,) = assemble(kernel, [ids], arrays, [shape], shape)
    message = pair(pick(last, None), starts[last:], rows, tile, share, last)
    from_near = lax.ppermute(message, "sub", near)
    kernel = functools.partial(rest_kernel, starts=starts[-1:], parts=rows, tile=tile, low_tile=last)
    arrays = [base] + pick(-1, None)
    base, weights = assemble(kernel, [ids], arrays, [shape, (PAIR, count, 8, tile)], shape)
    (out,) = assemble(finish_kernel, [], [base, from_near, weights], [shape], None)
    return out[None]


def solution(mesh):
    return jax.shard_map(
        shards,
        mesh=mesh,
        in_specs=(
            P("sub", "row", None, None, None),
            P("sub", "row", None, None),
            P("sub", "row", None),
            P("sub", "row", None),
            P("sub", None, "row", None),
            P(),
        ),
        out_specs=P("sub", None, "row", None),
        check_vma=False,
    )
```
